32 devices in a mesh: head: 8 (over z, x), client: 4 (over y, core).
Axes of the slice: x: 2, y: 2, z: 4, core: 2. Of those that a mesh axis runs over, the one named last changes fastest.
Arguments:
- client_ids: int32 [32], replicated, may hold values from 0 to 127, as said below
- client_table: bfloat16 [128, 256], replicated, may hold values from -6 to 6
- in_weight: bfloat16 [256, 4096], P(None, 'client'), may hold values from -0.375 to 0.375
- in_bias: float32 [4096], P('client'), may hold values from -3 to 3
- head_weight: bfloat16 [4096, 131072], P('client', 'head'), may hold values from -0.09375 to 0.09375
- tokens: int32 [32, 256], P(('head', 'client')), may hold values from 0 to 255
- labels: int32 [32, 256], P(('head', 'client')), may hold values from 0 to 255
- byte_table: bfloat16 [256, 4096], P(None, 'client'), may hold values from -5.5 to 6.7
- out_table: bfloat16 [256, 4096], P(None, 'client'), may hold values from -5.625 to 5.625
Outputs:
- head_grad: bfloat16 [4096, 131072], P('client', 'head')
- in_grad: float32 [256, 4096], P(None, 'client')
- losses: float32 [32], P(('head', 'client'))
The draws below stay inside these ranges and needn't reach their ends.
Inputs may be any that keep to these rules, and one draw needn't show every extreme that they name: `client_ids`: distinct population indices.
All inputs are finite; a program needn't handle non-finite values.
Results may differ from the reference program's by a relative error of at most 0.0085.
Values may be sent and summed in bfloat16 or wider, within the bound.
A program may use at most 128 MiB of HBM per device.

```python
import jax
import jax.numpy as jnp
from jax import lax

H = 4096
E = 256
D = 4096
VOCAB = 256
SEQ = 256
CLIENTS = 32
NPOP = 128
P_SIZE = 131072


def draw_client_ids(key, part):
    return jax.random.permutation(key, NPOP)[:CLIENTS].astype(jnp.int32)


def table_parts(key):
    noise_key = jax.random.fold_in(jax.random.fold_in(key, 7), 0)
    values = jnp.clip(jax.random.normal(noise_key, (VOCAB, D), jnp.float32), -5.5, 5.5)
    return values


def draw_byte_table(key, part):
    values = table_parts(key)
    return values.astype(jnp.bfloat16)


def draw_out_table(key, part):
    values = jnp.clip(jax.random.normal(jax.random.fold_in(key, 11), (VOCAB, D), jnp.float32), -5.5, 5.5)
    return values.astype(jnp.bfloat16)


def touch_ends(entries, key, low, largest):
    spot = [jax.random.randint(jax.random.fold_in(key, axis), (), 0, length) for axis, length in enumerate(entries.shape)]
    widest = entries.shape.index(max(entries.shape))
    next_to = spot[:widest] + [(spot[widest] + 1) % entries.shape[widest]] + spot[widest + 1:]
    return entries.at[tuple(spot)].set(low).at[tuple(next_to)].set(largest)


def level_of(stream_key, dims, pieces, low, top_value):
    level, own = 1.0, jax.random.fold_in(stream_key, 6)
    for position, shards_of in pieces:
        heights = jnp.exp(jax.random.uniform(jax.random.fold_in(own, position), (shards_of,), jnp.float32, low / len(pieces), top_value / len(pieces)))
        level = level * jnp.repeat(heights, dims[position] // shards_of).reshape([-1 if axis == position else 1 for axis in range(len(dims))])
    return level


def scatter_about(own_key, dims, scale, limit, shards=(), held_as=jnp.bfloat16):
    loudness = level_of(own_key, dims, shards, -0.22, 0.18) if shards else 1.0
    entries = jax.random.normal(own_key, dims, jnp.float32) * scale * loudness
    return jnp.minimum(jnp.maximum(entries, -limit), limit).astype(held_as)


def setup_inputs(seed: int = 0) -> dict:
    keys = jax.random.split(jax.random.key(seed), 10)
    client_ids = draw_client_ids(jax.random.fold_in(keys[9], 71), 0)
    client_table = scatter_about(keys[1], (NPOP, E), 1.0, 6.0)
    in_weight = scatter_about(keys[2], (E, H), E ** -0.5, 0.375, ((1, 4),))
    in_bias = scatter_about(keys[3], (H,), 0.5, 3.0, ((0, 4),), jnp.float32)
    head_weight = scatter_about(keys[4], (H, P_SIZE), H ** -0.5, 0.09375, ((0, 4), (1, 8)))
    tokens = touch_ends(jax.random.randint(keys[5], (CLIENTS, SEQ), 0, VOCAB), jax.random.fold_in(keys[5], 1), 0, VOCAB - 1).astype(jnp.int32)
    labels = touch_ends(jax.random.randint(keys[6], (CLIENTS, SEQ), 0, VOCAB), jax.random.fold_in(keys[6], 1), 0, VOCAB - 1).astype(jnp.int32)
    byte_table = draw_byte_table(jax.random.fold_in(keys[9], 71), 0)
    out_table = draw_out_table(jax.random.fold_in(keys[9], 71), 0)
    return dict(client_ids=client_ids, client_table=client_table, in_weight=in_weight, in_bias=in_bias, head_weight=head_weight, tokens=tokens, labels=labels, byte_table=byte_table, out_table=out_table)


EPSILON = 1e-06
learn_rate = 0.1

def client_loss(factor_a, factor_b, inputs, label_row, out_table):
    depth = factor_a.shape[0]
    rank_size = factor_a.shape[1]
    normed_in = inputs * lax.rsqrt(lax.optimization_barrier(jnp.mean(inputs * inputs, -1, keepdims=True)) + EPSILON)
    low_rank = jnp.dot(normed_in, factor_a, precision=lax.Precision.HIGHEST)
    adapted = inputs + jnp.dot(low_rank, factor_b, precision=lax.Precision.HIGHEST) / jnp.sqrt(jnp.float32(depth * rank_size))
    normed = (adapted * lax.rsqrt(lax.optimization_barrier(jnp.mean(adapted * adapted, -1, keepdims=True)) + EPSILON)).astype(jnp.bfloat16)
    logits = lax.dot_general(normed, out_table, (((1,), (1,)), ((), ())), preferred_element_type=jnp.float32)
    logits = logits * (4.0 / jnp.sqrt(jnp.float32(depth)))
    log_total = jax.nn.logsumexp(logits, -1)
    vocab_ids = lax.broadcasted_iota(jnp.int32, logits.shape, 1)
    picked = lax.optimization_barrier(jnp.sum(jnp.where(vocab_ids == label_row[:, None], logits, 0.0), -1))
    return jnp.sum(log_total - picked)

def train_client(factor_row, token_row, label_row, byte_table, out_table):
    depth = byte_table.shape[1]
    split_at = factor_row.shape[0] // 2
    rank_size = split_at // depth
    start_a = factor_row[:split_at].reshape(depth, rank_size).astype(jnp.float32)
    start_b = factor_row[split_at:].reshape(rank_size, depth).astype(jnp.float32)
    onehot = (token_row[:, None] == lax.broadcasted_iota(jnp.int32, (token_row.shape[0], byte_table.shape[0]), 1)).astype(jnp.bfloat16)
    inputs = jnp.dot(onehot, byte_table, preferred_element_type=jnp.float32)
    loss_grad = jax.value_and_grad(client_loss, argnums=(0, 1))
    first_loss, (grad_a, grad_b) = loss_grad(start_a, start_b, inputs, label_row, out_table)
    middle_a = start_a - learn_rate * grad_a
    middle_b = start_b - learn_rate * grad_b
    second_loss, (grad_a, grad_b) = loss_grad(middle_a, middle_b, inputs, label_row, out_table)
    final_a = middle_a - learn_rate * grad_a
    final_b = middle_b - learn_rate * grad_b
    deltas = jnp.concatenate([(final_a - start_a).reshape(-1), (final_b - start_b).reshape(-1)]).astype(jnp.bfloat16)
    return (deltas, first_loss / token_row.shape[0])

def reference(client_ids, client_table, in_weight, in_bias, head_weight, tokens, labels, byte_table, out_table):
    chosen = client_table[client_ids]
    preact = jnp.dot(chosen, in_weight, preferred_element_type=jnp.float32) + in_bias
    hidden = jnp.maximum(preact, 0.0).astype(jnp.bfloat16)
    factors = jnp.dot(hidden, head_weight, preferred_element_type=jnp.float32).astype(jnp.bfloat16)
    blocks = CLIENTS // 8

    def run_block(record):
        return jax.vmap(lambda fac, tok, lab: train_client(fac, tok, lab, byte_table, out_table))(record[0], record[1], record[2])
    deltas, losses = lax.map(run_block, (factors.reshape(blocks, 8, -1), tokens.reshape(blocks, 8, -1), labels.reshape(blocks, 8, -1)))
    deltas = deltas.reshape(CLIENTS, -1)
    losses = losses.reshape(CLIENTS)
    head_grad = lax.dot_general(hidden, deltas, (((0,), (0,)), ((), ())), preferred_element_type=jnp.float32).astype(jnp.bfloat16)
    hidden_back = lax.dot_general(deltas, head_weight, (((1,), (1,)), ((), ())), preferred_element_type=jnp.float32)
    masked = jnp.where(preact > 0, hidden_back, 0.0)
    in_grad = lax.dot_general(chosen.astype(jnp.float32), masked, (((0,), (0,)), ((), ())), precision=lax.Precision.HIGHEST)
    return (head_grad, in_grad, losses)
```

```python
import functools

import jax
import jax.numpy as jnp
from jax import lax
from jax.experimental import pallas as pl
from jax.experimental.pallas import tpu as pltpu
from jax.sharding import PartitionSpec as P

EPSILON = 1e-06
learn_rate = 0.1
FULL = lax.Precision.HIGHEST
LANES = 128
PIECE_ROWS = 16
TABLE_PIECES = 8
HIGH_VMEM = 62 * 1024 * 1024
F32 = jnp.float32
BF16 = jnp.bfloat16


def mm(x, y, over_x=1, over_y=0):
    return lax.dot_general(
        x, y, (((over_x,), (over_y,)), ((), ())), precision=FULL, preferred_element_type=jnp.float32
    )


def exact(x, y, over_x, over_y):
    return lax.dot_general(
        x, y, (((over_x,), (over_y,)), ((), ())), preferred_element_type=jnp.float32
    )


def halves(x):
    top = lax.reduce_precision(x, 8, 7)
    rest = x - top
    return jnp.concatenate([top.astype(jnp.bfloat16), rest.astype(jnp.bfloat16)], 1)


def inner_step(u, n_in, m_out, k_bb, gram_io, mean_in, pair_count, depth, scale):
    uk = mm(u, k_bb)
    z = gram_io + scale * mm(u, m_out, 1, 1)
    q = mean_in + jnp.sum(u * (2.0 * scale * n_in + (scale * scale) * uk), -1, keepdims=True) / depth
    r = lax.rsqrt(q + EPSILON)
    kappa = 4.0 / jnp.sqrt(jnp.float32(depth))
    logits = (kappa * r) * z
    top = jnp.max(logits, -1, keepdims=True)
    raised = jnp.exp(logits - top)
    total = jnp.sum(raised, -1, keepdims=True)
    row_count = jnp.sum(pair_count, -1, keepdims=True)
    loss = jnp.sum(row_count * (jnp.log(total) + top)) - jnp.sum(pair_count * logits)
    slope = row_count * (raised / total) - pair_count
    dz = (kappa * r) * slope
    dr = kappa * jnp.sum(slope * z, -1, keepdims=True)
    e = dr * (-1.0 / depth) * (r * r * r)
    gu = scale * (mm(dz, m_out) + e * (n_in + scale * uk))
    w = mm(dz, u, 0, 0)
    x = e * u
    y = mm(u, x, 0, 0)
    return loss, gu, w, x, y


def table_products(byte_full, out_full):
    depth = byte_full.shape[1]
    gram_ii = exact(byte_full, byte_full, 1, 1)
    gram_io = exact(byte_full, out_full, 1, 1)
    gram_oo = exact(out_full, out_full, 1, 1)
    size = gram_ii.shape[0]
    diagonal = lax.broadcasted_iota(jnp.int32, (size, size), 0) == lax.broadcasted_iota(
        jnp.int32, (size, size), 1
    )
    mean_in = jnp.sum(jnp.where(diagonal, gram_ii, 0.0), -1, keepdims=True) / depth
    return gram_ii, gram_io, gram_oo, mean_in


def train_client(factor_row, token_row, label_row, byte_full, out_full, products):
    gram_ii, gram_io, gram_oo, mean_in = products
    vocab, depth = byte_full.shape
    split_at = factor_row.shape[0] // 2
    rank = split_at // depth
    scale = 1.0 / jnp.sqrt(jnp.float32(depth * rank))
    a0 = factor_row[:split_at].reshape(depth, rank)
    b0 = factor_row[split_at:].reshape(rank, depth)
    ids = lax.broadcasted_iota(jnp.int32, (vocab, token_row.shape[0]), 0)
    pair_count = exact(
        (ids == token_row[None, :]).astype(jnp.bfloat16),
        (ids == label_row[None, :]).astype(jnp.bfloat16),
        1,
        1,
    )
    rn = lax.rsqrt(mean_in + EPSILON)
    u0 = rn * exact(byte_full, a0, 1, 0)
    n0 = exact(byte_full, b0, 1, 1)
    m0 = exact(out_full, b0, 1, 1)
    k0 = exact(b0, b0, 1, 1)
    fixed = (gram_io, mean_in, pair_count, depth, scale)
    first_loss, gu0, w0, x0, y0 = inner_step(u0, n0, m0, k0, *fixed)
    rate = learn_rate * scale
    w0, x0, y0 = -rate * w0, -rate * x0, (-rate * scale) * y0
    u1 = u0 - learn_rate * rn * mm(gram_ii, rn * gu0)
    n1 = n0 + mm(gram_io, w0) + mm(gram_ii, x0) + mm(n0, y0)
    m1 = m0 + mm(gram_oo, w0) + mm(gram_io, x0, 0, 0) + mm(m0, y0)
    cross = k0 + mm(y0, k0, 0, 0) + mm(w0, m0, 0, 0) + mm(x0, n0, 0, 0)
    k1 = cross + mm(cross, y0) + mm(m1, w0, 0, 0) + mm(n1, x0, 0, 0)
    _, gu1, w1, x1, y1 = inner_step(u1, n1, m1, k1, *fixed)
    w1, x1, y1 = -rate * w1, -rate * x1, (-rate * scale) * y1
    ga = (-learn_rate) * rn * (gu0 + gu1)
    wf = w0 + w1 + mm(w0, y1)
    xf = x0 + x1 + mm(x0, y1)
    yf = y0 + y1 + mm(y0, y1)
    da = exact(byte_full, halves(ga), 0, 0)
    da = da[:, :rank] + da[:, rank:]
    db = (
        exact(halves(wf), out_full, 0, 0)
        + exact(halves(xf), byte_full, 0, 0)
        + exact(halves(yf), b0, 0, 0)
    )
    db = db[:rank] + db[rank:]
    deltas = jnp.concatenate([da.astype(jnp.bfloat16).reshape(-1), db.astype(jnp.bfloat16).reshape(-1)])
    return deltas, first_loss / token_row.shape[0]


def to_head(h):
    return {"head": h}


def to_client(g):
    return {"client": g}


def remote(src, dst, send, recv, device):
    return pltpu.make_async_remote_copy(
        src_ref=src,
        dst_ref=dst,
        send_sem=send,
        recv_sem=recv,
        device_id=device,
        device_id_type=pl.DeviceIdType.MESH,
    )


def meet(heads, h, g):
    sem = pltpu.get_barrier_semaphore()

    @pl.loop(1, heads)
    def _(i):
        pl.semaphore_signal(
            sem, inc=1, device_id=to_head(lax.rem(h + i, heads)), device_id_type=pl.DeviceIdType.MESH
        )

    for other in (g ^ 1, g ^ 2):
        pl.semaphore_signal(
            sem, inc=1, device_id=to_client(other), device_id_type=pl.DeviceIdType.MESH
        )
    pl.semaphore_wait(sem, heads + 1)


def forward_kernel(
    heads, steps, ids, client_table, in_weight, in_bias, head_weight, byte_table, out_table,
    factors, tables, hidden_out, preact_out, chosen_out,
    wv, ct, iw, ib, tv, chosen_v, preact_v, hidden_v, s1, r1, k2, s2, r2, s3,
    w_sem, in_sem, out_sem, own_sem, p_send, p_recv, y_send, y_recv, f_send, f_recv,
    t_own_send, t_own_recv, t_send, t_recv, t_pair_send, t_pair_recv, tl_sem,
):
    h, g = lax.axis_index("head"), lax.axis_index("client")
    core, far = g & 1, g >> 1
    pair, peer = g ^ 1, g ^ 2
    x_side, z_side = h ^ 1, h ^ 2
    clients = hidden_v.shape[0]
    group = clients // 4
    block_rows = steps * PIECE_ROWS
    width = PIECE_ROWS * LANES
    vocab = tv.shape[1]
    part = vocab // 4 // (TABLE_PIECES // 2)

    small = [
        pltpu.make_async_copy(client_table, ct, in_sem.at[0]),
        pltpu.make_async_copy(in_weight, iw, in_sem.at[1]),
        pltpu.make_async_copy(in_bias, ib, in_sem.at[2]),
        pltpu.make_async_copy(byte_table, tv.at[0], in_sem.at[3]),
        pltpu.make_async_copy(out_table, tv.at[1], in_sem.at[4]),
    ]
    for c in small:
        c.start()

    def w_copy(k):
        return pltpu.make_async_copy(
            head_weight.at[:, pl.ds(pl.multiple_of(k * width, width), width)], wv.at[k], w_sem.at[k]
        )

    @pl.loop(0, steps)
    def _(k):
        w_copy(k).start()

    for c in small:
        c.wait()
    population = lax.broadcasted_iota(jnp.int32, (clients, ct.shape[0]), 1)
    onehot = jnp.where(ids[...] == population, 1.0, 0.0).astype(BF16)
    chosen = jnp.dot(onehot, ct[...], preferred_element_type=F32).astype(BF16)
    chosen_v[...] = chosen
    preact = jnp.dot(chosen, iw[...], preferred_element_type=F32) + ib[...]
    preact_v[...] = preact
    hidden_v[...] = jnp.maximum(preact, 0.0).astype(BF16)

    meet(heads, h, g)

    quarter = [tables.at[t, g] for t in range(2)]

    def piece(t, owner_head, col):
        table = lax.div(t, TABLE_PIECES // 2)
        row = lax.rem(owner_head, 4) * (vocab // 4) + lax.rem(t, TABLE_PIECES // 2) * part
        return table, col, pl.ds(pl.multiple_of(row, part), part)

    own_to_out = [
        pltpu.make_async_copy(tv.at[t], quarter[t], tl_sem.at[t]) for t in range(2)
    ]
    own_to_pair = [
        remote(tv.at[t], quarter[t], t_own_send.at[t], t_own_recv.at[t], to_client(pair))
        for t in range(2)
    ]
    for c in own_to_out + own_to_pair:
        c.start()

    def t_peer(t):
        table, col, rows = piece(t, h, g)
        return remote(
            tv.at[table, rows], tables.at[table, col, rows],
            t_send.at[0, t], t_recv.at[0, t], to_client(peer),
        )

    def t_side(kind, t):
        table, col, rows = piece(t, h, peer)
        ref = tables.at[table, col, rows]
        return remote(ref, ref, t_send.at[kind, t], t_recv.at[kind, t], to_head((x_side, z_side)[kind - 1]))

    def t_relay(t, odd):
        table, col, rows = piece(t, x_side if odd else z_side, peer)
        ref = tables.at[table, col, rows]
        return remote(ref, ref, t_send.at[3, t], t_recv.at[3, t], to_head(z_side if odd else x_side))

    def t_pair(kind, t):
        owner = (h, x_side, z_side, h ^ 3)[kind]
        table, col, rows = piece(t, owner, peer)
        ref = tables.at[table, col, rows]
        return remote(ref, ref, t_pair_send.at[kind, t], t_pair_recv.at[kind, t], to_client(pair))

    def to_pair(k):
        return remote(
            s1.at[k, pl.ds((1 - core) * 2 * group, 2 * group)], r1.at[k],
            p_send.at[k], p_recv.at[k], to_client(pair),
        )

    def to_peer(k):
        return remote(s2.at[k], r2.at[k], y_send.at[k], y_recv.at[k], to_client(peer))

    def rows_of(head, k):
        return pl.ds(pl.multiple_of(head * block_rows + k * PIECE_ROWS, PIECE_ROWS), PIECE_ROWS)

    def to_owner(k, i):
        other = lax.rem(h + i, heads)
        return remote(
            s3.at[k, other], factors.at[rows_of(h, k)],
            f_send.at[k, other], f_recv.at[k, h], to_head(other),
        )

    def from_owner(k, i):
        other = lax.rem(h + i, heads)
        return remote(
            s3.at[k, other], factors.at[rows_of(other, k)],
            f_send.at[k, other], f_recv.at[k, other], to_head(other),
        )

    def own_piece(k):
        return pltpu.make_async_copy(s3.at[k, h], factors.at[rows_of(h, k)], own_sem.at[k])

    small_out = [
        pltpu.make_async_copy(hidden_v, hidden_out, out_sem.at[0]),
        pltpu.make_async_copy(preact_v, preact_out, out_sem.at[1]),
        pltpu.make_async_copy(chosen_v, chosen_out, out_sem.at[2]),
    ]
    for c in small_out:
        c.start()

    def fwd_stage(k):
        w_copy(k).wait()
        for n in range(width // 512):
            out = jnp.dot(
                hidden_v[...], wv[k, :, n * 512 : (n + 1) * 512], preferred_element_type=F32
            )
            for q in range(4):
                s1[k, :, n * 4 + q, :] = out[:, q * LANES : (q + 1) * LANES]
        to_pair(k).start()

    def pair_stage(k):
        to_pair(k).wait_recv()
        theirs = core * 2 * group + (1 - far) * group
        mine = core * 2 * group + far * group
        s2[k] = (s1[k, pl.ds(theirs, group)] + r1[k, pl.ds((1 - far) * group, group)]).astype(BF16)
        to_peer(k).start()
        k2[k] = s1[k, pl.ds(mine, group)] + r1[k, pl.ds(far * group, group)]

    def peer_stage(k):
        to_peer(k).wait_recv()
        s3[k] = (k2[k] + r2[k].astype(F32)).astype(BF16)
        own_piece(k).start()

        @pl.loop(1, heads)
        def _(i):
            to_owner(k, i).start()

    def table_stage(k):
        @pl.when(k < TABLE_PIECES // 2)
        def _():
            t_peer(2 * k).start()
            t_peer(2 * k + 1).start()

        for lag in range(2):
            t0 = k - 3 - lag

        @pl.when((k >= 3) & (k < 3 + TABLE_PIECES))
        def _():
            t = k - 3
            t_peer(t).wait_recv()
            t_side(1, t).start()
            t_side(2, t).start()
            t_pair(0, t).start()

        @pl.when((k >= 5) & (k < 5 + TABLE_PIECES))
        def _():
            t = k - 5
            t_side(1, t).wait_recv()
            t_side(2, t).wait_recv()

            @pl.when(lax.rem(t, 2) == 1)
            def _():
                t_relay(t, True).start()

            @pl.when(lax.rem(t, 2) == 0)
            def _():
                t_relay(t, False).start()

            t_pair(1, t).start()
            t_pair(2, t).start()

        @pl.when((k >= 7) & (k < 7 + TABLE_PIECES))
        def _():
            t = k - 7
            t_relay(t, False).wait_recv()
            t_pair(3, t).start()

    @pl.loop(0, max(steps + 3, TABLE_PIECES + 7))
    def _(k):
        @pl.when(k < steps)
        def _():
            fwd_stage(k)

        @pl.when((k >= 1) & (k < steps + 1))
        def _():
            pair_stage(k - 1)

        @pl.when((k >= 3) & (k < steps + 3))
        def _():
            peer_stage(k - 3)

        table_stage(k)

    @pl.loop(0, steps)
    def _(k):
        to_pair(k).wait_send()
        to_peer(k).wait_send()
        own_piece(k).wait()

        @pl.loop(1, heads)
        def _(i):
            to_owner(k, i).wait_send()
            from_owner(k, i).wait_recv()

    for c in own_to_out:
        c.wait()
    for c in own_to_pair:
        c.wait_send()
        c.wait_recv()
    for c in small_out:
        c.wait()

    @pl.loop(0, TABLE_PIECES)
    def _(t):
        t_peer(t).wait_send()
        t_side(1, t).wait_send()
        t_side(2, t).wait_send()
        t_relay(t, False).wait_send()
        for kind in range(4):
            t_pair(kind, t).wait_send()
            t_pair(kind, t).wait_recv()


def back_kernel(
    heads, steps, deltas, head_weight, spread, back_parts,
    wv, e, x, db, acc, b1s, b1r, tot, b2,
    w_sem, own_sem, d_send, d_recv, y_send, y_recv, p_send, p_recv, q_send, q_recv,
    b_send, b_recv, c_send, c_recv, o_sem, z_sem,
):
    h, g = lax.axis_index("head"), lax.axis_index("client")
    pair, peer = g ^ 1, g ^ 2
    width = PIECE_ROWS * LANES
    block_rows = steps * PIECE_ROWS
    clients = db.shape[0] if db.ndim == 2 else db.shape[1]
    group = clients // 4
    each = clients // heads
    units = acc.shape[0]

    def place(c):
        return (c & 1) * 2 + (c >> 1)

    def w_copy(k):
        return pltpu.make_async_copy(
            head_weight.at[:, pl.ds(pl.multiple_of(k * width, width), width)], wv.at[k], w_sem.at[k]
        )

    def rows_of(head, k):
        return pl.ds(pl.multiple_of(head * block_rows + k * PIECE_ROWS, PIECE_ROWS), PIECE_ROWS)

    def own_piece(k):
        return pltpu.make_async_copy(deltas.at[rows_of(h, k)], e.at[place(g), k, h], own_sem.at[k])

    def to_holder(k, i):
        other = lax.rem(h + i, heads)
        return remote(
            deltas.at[rows_of(other, k)], e.at[place(g), k, h],
            d_send.at[k, other], d_recv.at[k, h], to_head(other),
        )

    def from_owner(k, i):
        other = lax.rem(h + i, heads)
        return remote(
            deltas.at[rows_of(other, k)], e.at[place(g), k, other],
            d_send.at[k, other], d_recv.at[k, other], to_head(other),
        )

    def to_peer(k):
        ref = e.at[place(g), k]
        return remote(ref, ref, y_send.at[k], y_recv.at[k], to_client(peer))

    def from_peer(k):
        ref = e.at[place(peer), k]
        return remote(ref, ref, y_send.at[k], y_recv.at[k], to_client(peer))

    def to_pair(k):
        ref = e.at[place(g), k]
        return remote(ref, ref, p_send.at[k], p_recv.at[k], to_client(pair))

    def on_to_pair(k):
        ref = e.at[place(peer), k]
        return remote(ref, ref, q_send.at[k], q_recv.at[k], to_client(pair))

    meet(heads, h, g)

    @pl.loop(0, steps)
    def _(k):
        own_piece(k).start()

        @pl.loop(1, heads)
        def _(i):
            to_holder(k, i).start()

    @pl.loop(0, steps)
    def _(k):
        w_copy(k).start()

    acc[...] = jnp.zeros_like(acc)

    def spread_out(k):
        return pltpu.make_async_copy(
            db.at[k], spread.at[:, pl.ds(pl.multiple_of(k * width, width), width)], o_sem.at[k]
        )

    @pl.loop(0, steps + 2)
    def _(k):
        @pl.when(k < steps)
        def _():
            own_piece(k).wait()

            @pl.loop(1, heads)
            def _(i):
                from_owner(k, i).wait_recv()

            to_peer(k).start()
            to_pair(k).start()

        @pl.when((k >= 1) & (k < steps + 1))
        def _():
            from_peer(k - 1).wait_recv()
            on_to_pair(k - 1).start()

        @pl.when(k >= 2)
        def _():
            j = k - 2
            to_pair(j).wait_recv()
            on_to_pair(j).wait_recv()
            for c in range(4):
                x[c * group : (c + 1) * group] = e[c, j].astype(F32)
            for q in range(PIECE_ROWS):
                db[j, :, q * LANES : (q + 1) * LANES] = x[:, q, :].astype(BF16)
            spread_out(j).start()
            w_copy(j).wait()
            acc[...] += lax.dot_general(
                wv[j], db[j], (((1,), (1,)), ((), ())), preferred_element_type=F32
            )

    flat = acc[...].T
    for j in range(heads):
        for b in range(units // LANES):
            b1s[j, b * each : (b + 1) * each, :] = flat[
                j * each : (j + 1) * each, b * LANES : (b + 1) * LANES
            ]

    def part_to(i):
        other = lax.rem(h + i, heads)
        return remote(b1s.at[other], b1r.at[h], b_send.at[other], b_recv.at[h], to_head(other))

    def part_from(i):
        other = lax.rem(h + i, heads)
        return remote(b1s.at[other], b1r.at[other], b_send.at[other], b_recv.at[other], to_head(other))

    def sum_to(i):
        other = lax.rem(h + i, heads)
        return remote(tot, b2.at[h], c_send.at[other], c_recv.at[h], to_head(other))

    def sum_from(i):
        other = lax.rem(h + i, heads)
        return remote(tot, b2.at[other], c_send.at[other], c_recv.at[other], to_head(other))

    @pl.loop(1, heads)
    def _(i):
        part_to(i).start()

    tot[...] = b1s[h]

    @pl.loop(1, heads)
    def _(i):
        part_from(i).wait_recv()
        tot[...] += b1r[lax.rem(h + i, heads)]

    b2[h] = tot[...]

    @pl.loop(1, heads)
    def _(i):
        sum_to(i).start()

    @pl.loop(0, steps)
    def _(k):
        to_peer(k).wait_send()
        to_pair(k).wait_send()
        on_to_pair(k).wait_send()
        spread_out(k).wait()

        @pl.loop(1, heads)
        def _(i):
            to_holder(k, i).wait_send()

    @pl.loop(1, heads)
    def _(i):
        part_to(i).wait_send()
        sum_to(i).wait_send()
        sum_from(i).wait_recv()

    last = pltpu.make_async_copy(b2, back_parts, z_sem)
    last.start()
    last.wait()


def grad_kernel(heads, hidden, spread, back_parts, preact, chosen, head_grad, in_grad, turned, hb):
    clients, units = hidden.shape
    each = clients // heads

    @pl.when(pl.program_id(0) == 0)
    def _():
        turned[...] = hidden[...].astype(F32).T.astype(BF16)
        for j in range(heads):
            for b in range(units // LANES):
                hb[j * each : (j + 1) * each, b * LANES : (b + 1) * LANES] = back_parts[
                    j, b * each : (b + 1) * each, :
                ]
        masked = jnp.where(preact[...] > 0, hb[...], 0.0)
        top = masked.astype(BF16)
        rest = masked - top.astype(F32)
        mid = rest.astype(BF16)
        low = (rest - mid.astype(F32)).astype(BF16)
        sel = chosen[...]
        total = jnp.zeros(in_grad.shape, F32)
        for term in (low, mid, top):
            total += lax.dot_general(sel, term, (((0,), (0,)), ((), ())), preferred_element_type=F32)
        in_grad[...] = total

    head_grad[...] = jnp.dot(turned[...], spread[...], preferred_element_type=F32).astype(BF16)


def local(
    client_ids, client_table, in_weight, in_bias, head_weight, tokens, labels, byte_table, out_table
):
    heads = lax.axis_size("head")
    groups = lax.axis_size("client")
    assert groups == 4 and tokens.shape[0] == 1 and heads % 4 == 0
    units, columns = head_weight.shape
    clients = client_ids.shape[0]
    embed = client_table.shape[1]
    vocab, share = byte_table.shape
    depth = share * groups
    width = PIECE_ROWS * LANES
    steps = columns // width
    rows = heads * columns // LANES
    group = clients // groups
    each = clients // heads
    part_rows = each * units // LANES
    any_spec = pl.BlockSpec(memory_space=pl.ANY)
    vmem_spec = pl.BlockSpec(memory_space=pltpu.VMEM)
    dma = pltpu.SemaphoreType.DMA

    ordered = client_ids.reshape(heads, 2, 2).transpose(2, 1, 0).reshape(clients, 1)
    factors, tables, hidden, preact, chosen = pl.pallas_call(
        functools.partial(forward_kernel, heads, steps),
        name="forward",
        out_shape=[
            jax.ShapeDtypeStruct((rows, LANES), BF16),
            jax.ShapeDtypeStruct((2, groups, vocab, share), BF16),
            jax.ShapeDtypeStruct((clients, units), BF16),
            jax.ShapeDtypeStruct((clients, units), F32),
            jax.ShapeDtypeStruct((clients, embed), BF16),
        ],
        in_specs=[vmem_spec] + [any_spec] * 6,
        out_specs=[any_spec] * 5,
        scratch_shapes=[
            pltpu.VMEM((steps, units, width), BF16),
            pltpu.VMEM(client_table.shape, BF16),
            pltpu.VMEM(in_weight.shape, BF16),
            pltpu.VMEM((1, units), F32),
            pltpu.VMEM((2, vocab, share), BF16),
            pltpu.VMEM((clients, embed), BF16),
            pltpu.VMEM((clients, units), F32),
            pltpu.VMEM((clients, units), BF16),
            pltpu.VMEM((steps, clients, PIECE_ROWS, LANES), F32),
            pltpu.VMEM((steps, 2 * group, PIECE_ROWS, LANES), F32),
            pltpu.VMEM((steps, group, PIECE_ROWS, LANES), F32),
            pltpu.VMEM((steps, group, PIECE_ROWS, LANES), BF16),
            pltpu.VMEM((steps, group, PIECE_ROWS, LANES), BF16),
            pltpu.VMEM((steps, group, PIECE_ROWS, LANES), BF16),
            dma((steps,)), dma((5,)), dma((3,)), dma((steps,)),
            dma((steps,)), dma((steps,)), dma((steps,)), dma((steps,)),
            dma((steps, heads)), dma((steps, heads)),
            dma((2,)), dma((2,)), dma((4, TABLE_PIECES)), dma((4, TABLE_PIECES)),
            dma((4, TABLE_PIECES)), dma((4, TABLE_PIECES)), dma((2,)),
        ],
        compiler_params=pltpu.CompilerParams(
            collective_id=0, has_side_effects=True, vmem_limit_bytes=HIGH_VMEM
        ),
    )(ordered, client_table, in_weight, in_bias.reshape(1, units), head_weight, byte_table, out_table)

    byte_full = tables[0].transpose(1, 0, 2).reshape(vocab, depth)
    out_full = tables[1].transpose(1, 0, 2).reshape(vocab, depth)
    products = table_products(byte_full, out_full)
    deltas, loss = train_client(factors.reshape(-1), tokens[0], labels[0], byte_full, out_full, products)
    deltas = deltas.reshape(rows, LANES)

    spread, back_parts = pl.pallas_call(
        functools.partial(back_kernel, heads, steps),
        name="back",
        out_shape=[
            jax.ShapeDtypeStruct((clients, columns), BF16),
            jax.ShapeDtypeStruct((heads, part_rows, LANES), F32),
        ],
        in_specs=[any_spec] * 2,
        out_specs=[any_spec] * 2,
        scratch_shapes=[
            pltpu.VMEM((steps, units, width), BF16),
            pltpu.VMEM((groups, steps, heads, PIECE_ROWS, LANES), BF16),
            pltpu.VMEM((clients, PIECE_ROWS, LANES), F32),
            pltpu.VMEM((steps, clients, width), BF16),
            pltpu.VMEM((units, clients), F32),
            pltpu.VMEM((heads, part_rows, LANES), F32),
            pltpu.VMEM((heads, part_rows, LANES), F32),
            pltpu.VMEM((part_rows, LANES), F32),
            pltpu.VMEM((heads, part_rows, LANES), F32),
            dma((steps,)), dma((steps,)), dma((steps, heads)), dma((steps, heads)),
            dma((steps,)), dma((steps,)), dma((steps,)), dma((steps,)), dma((steps,)), dma((steps,)),
            dma((heads,)), dma((heads,)), dma((heads,)), dma((heads,)), dma((steps,)), dma,
        ],
        compiler_params=pltpu.CompilerParams(
            collective_id=1, has_side_effects=True, vmem_limit_bytes=HIGH_VMEM
        ),
    )(deltas, head_weight)

    block = 1024
    fixed = lambda *shape: pl.BlockSpec(shape, lambda i: (0,) * len(shape))
    head_grad, in_grad = pl.pallas_call(
        functools.partial(grad_kernel, heads),
        name="grad",
        grid=(columns // block,),
        out_shape=[
            jax.ShapeDtypeStruct((units, columns), BF16),
            jax.ShapeDtypeStruct((embed, units), F32),
        ],
        in_specs=[
            fixed(clients, units),
            pl.BlockSpec((clients, block), lambda i: (0, i)),
            fixed(heads, part_rows, LANES),
            fixed(clients, units),
            fixed(clients, embed),
        ],
        out_specs=[pl.BlockSpec((units, block), lambda i: (0, i)), fixed(embed, units)],
        scratch_shapes=[pltpu.VMEM((units, clients), BF16), pltpu.VMEM((clients, units), F32)],
        compiler_params=pltpu.CompilerParams(vmem_limit_bytes=HIGH_VMEM),
    )(hidden, spread, back_parts, preact, chosen)
    return head_grad, in_grad, loss.reshape(1)


def solution(mesh):
    placed = (
        P(),
        P(),
        P(None, "client"),
        P("client"),
        P("client", "head"),
        P(("head", "client"), None),
        P(("head", "client"), None),
        P(None, "client"),
        P(None, "client"),
    )
    return jax.shard_map(
        local,
        mesh=mesh,
        in_specs=placed,
        out_specs=(P("client", "head"), P(None, "client"), P(("head", "client"))),
        check_vma=False,
    )
```

```python
import functools

import jax
import jax.numpy as jnp
from jax import lax
from jax.experimental import pallas as pl
from jax.experimental.pallas import tpu as pltpu
from jax.sharding import PartitionSpec as P

EPSILON = 1e-06
learn_rate = 0.1
LANES = 128
PIECE_ROWS = 16
TABLE_PIECES = 8
HIGH_VMEM = 62 * 1024 * 1024
F32 = jnp.float32
BF16 = jnp.bfloat16


def split(x):
    top = x.astype(BF16)
    return top, (x - top.astype(F32)).astype(BF16)


def mm(x, y, over_x=1, over_y=0):
    (x_top, x_low), (y_top, y_low) = split(x), split(y)
    return (
        exact(x_top, y_low, over_x, over_y)
        + exact(x_low, y_top, over_x, over_y)
        + exact(x_top, y_top, over_x, over_y)
    )


def exact(x, y, over_x, over_y):
    return lax.dot_general(
        x, y, (((over_x,), (over_y,)), ((), ())), preferred_element_type=jnp.float32
    )


def inner_step(u, n_in, m_out, k_bb, gram_io, mean_in, pair_count, depth, scale):
    uk = mm(u, k_bb)
    z = gram_io + scale * mm(u, m_out, 1, 1)
    q = mean_in + jnp.sum(u * (2.0 * scale * n_in + (scale * scale) * uk), -1, keepdims=True) / depth
    r = lax.rsqrt(q + EPSILON)
    kappa = 4.0 / float(depth) ** 0.5
    logits = (kappa * r) * z
    top = jnp.max(logits, -1, keepdims=True)
    raised = jnp.exp(logits - top)
    total = jnp.sum(raised, -1, keepdims=True)
    row_count = jnp.sum(pair_count, -1, keepdims=True)
    loss = jnp.sum(
        row_count * (jnp.log(total) + top) - jnp.sum(pair_count * logits, -1, keepdims=True), 0, keepdims=True
    )
    slope = row_count * (raised / total) - pair_count
    dz = (kappa * r) * slope
    dr = kappa * jnp.sum(slope * z, -1, keepdims=True)
    e = dr * (-1.0 / depth) * (r * r * r)
    gu = scale * (mm(dz, m_out) + e * (n_in + scale * uk))
    w = mm(dz, u, 0, 0)
    x = e * u
    y = mm(u, x, 0, 0)
    return loss, gu, w, x, y


def table_products(tables):
    groups = tables.shape[1]

    def gram(left, right):
        total = exact(tables[left, 0], tables[right, 0], 1, 1)
        for c in range(1, groups):
            total += exact(tables[left, c], tables[right, c], 1, 1)
        return total

    return gram(0, 0), gram(0, 1), gram(1, 1)


def token_pairs(token_row, label_row, vocab):
    ids = lax.broadcasted_iota(jnp.int32, (vocab, token_row.shape[1]), 0)
    return exact(
        jnp.where(ids == token_row, 1.0, 0.0).astype(BF16),
        jnp.where(ids == label_row, 1.0, 0.0).astype(BF16),
        1,
        1,
    )


def train(factors, flat, spaced, b0, loss_ref, deltas, tables, grams, pair_count):
    gram_ii_ref, gram_io_ref, gram_oo_ref = grams
    groups, vocab, share = tables.shape[1:]
    depth = groups * share
    rows = factors.shape[0]
    rank = rows * LANES // (2 * depth)
    per_row = LANES // rank
    across = depth // LANES
    half = rows // 2
    scale = 1.0 / float(depth * rank) ** 0.5

    flat[...] = factors[...].astype(F32)
    lane = lax.broadcasted_iota(jnp.int32, (half // groups, per_row, LANES), 2)
    sub = lax.broadcasted_iota(jnp.int32, (half // groups, per_row, LANES), 1)
    here = lane // rank == sub
    for c in range(groups):
        q = half // groups
        wide = jnp.broadcast_to(flat[c * q : (c + 1) * q][:, None, :], (q, per_row, LANES))
        spaced[c * share : (c + 1) * share] = jnp.where(here, wide, 0.0).reshape(share, LANES).astype(BF16)
    for n in range(across):
        b0[:, n * LANES : (n + 1) * LANES] = flat[pl.ds(half + n, rank, stride=across), :].astype(BF16)

    def over_depth(f):
        total = f(0)
        for c in range(1, groups):
            total += f(c)
        return total

    cols = lambda c: slice(c * share, (c + 1) * share)
    folded = over_depth(lambda c: exact(tables[0, c], spaced[cols(c)], 1, 0))
    fold = jnp.where(
        lax.broadcasted_iota(jnp.int32, (LANES, rank), 0) % rank
        == lax.broadcasted_iota(jnp.int32, (LANES, rank), 1),
        1.0,
        0.0,
    )
    gram_ii, gram_io, gram_oo = gram_ii_ref[...], gram_io_ref[...], gram_oo_ref[...]
    diagonal = lax.broadcasted_iota(jnp.int32, (vocab, vocab), 0) == lax.broadcasted_iota(
        jnp.int32, (vocab, vocab), 1
    )
    mean_in = jnp.sum(jnp.where(diagonal, gram_ii, 0.0), -1, keepdims=True) / depth
    rn = lax.rsqrt(mean_in + EPSILON)
    u0 = rn * mm(folded, fold)
    n0 = over_depth(lambda c: exact(tables[0, c], b0[:, cols(c)], 1, 1))
    m0 = over_depth(lambda c: exact(tables[1, c], b0[:, cols(c)], 1, 1))
    k0 = exact(b0[...], b0[...], 1, 1)
    counts = pair_count[...]
    fixed = (gram_io, mean_in, counts, depth, scale)
    first_loss, gu0, w0, x0, y0 = inner_step(u0, n0, m0, k0, *fixed)
    loss_ref[...] = jnp.broadcast_to(first_loss, loss_ref.shape)
    rate = learn_rate * scale
    w0, x0, y0 = -rate * w0, -rate * x0, (-rate * scale) * y0
    u1 = u0 - learn_rate * rn * mm(gram_ii, rn * gu0)
    n1 = n0 + mm(gram_io, w0) + mm(gram_ii, x0) + mm(n0, y0)
    m1 = m0 + mm(gram_oo, w0) + mm(gram_io, x0, 0, 0) + mm(m0, y0)
    cross = k0 + mm(y0, k0, 0, 0) + mm(w0, m0, 0, 0) + mm(x0, n0, 0, 0)
    k1 = cross + mm(cross, y0) + mm(m1, w0, 0, 0) + mm(n1, x0, 0, 0)
    _, gu1, w1, x1, y1 = inner_step(u1, n1, m1, k1, *fixed)
    w1, x1, y1 = -rate * w1, -rate * x1, (-rate * scale) * y1
    ga = (-learn_rate) * rn * (gu0 + gu1)
    wf = w0 + w1 + mm(w0, y1)
    xf = x0 + x1 + mm(x0, y1)
    yf = y0 + y1 + mm(y0, y1)

    repeat = jnp.where(
        lax.broadcasted_iota(jnp.int32, (rank, LANES), 1) % rank
        == lax.broadcasted_iota(jnp.int32, (rank, LANES), 0),
        1.0,
        0.0,
    ).astype(BF16)
    ga_top, ga_low = (exact(t, repeat, 1, 0).astype(BF16) for t in split(ga))
    for c in range(groups):
        q = half // groups
        wide = exact(tables[0, c], ga_top, 0, 0) + exact(tables[0, c], ga_low, 0, 0)
        flat[c * q : (c + 1) * q] = jnp.sum(
            jnp.where(here, wide.reshape(q, per_row, LANES), 0.0), axis=1
        )
    parts = [jnp.concatenate([t.T for t in split(v)], 0) for v in (wf, xf, yf)]
    for c in range(groups):
        db = (
            exact(parts[0], tables[1, c], 1, 0)
            + exact(parts[1], tables[0, c], 1, 0)
            + exact(parts[2], b0[:, cols(c)], 1, 0)
        )
        db = db[:rank] + db[rank:]
        for n in range(share // LANES):
            flat[pl.ds(half + c * (share // LANES) + n, rank, stride=across), :] = db[
                :, n * LANES : (n + 1) * LANES
            ]
    deltas[...] = flat[...].astype(BF16)


def to_head(h):
    return {"head": h}


def to_client(g):
    return {"client": g}


def remote(src, dst, send, recv, device):
    return pltpu.make_async_remote_copy(
        src_ref=src,
        dst_ref=dst,
        send_sem=send,
        recv_sem=recv,
        device_id=device,
        device_id_type=pl.DeviceIdType.MESH,
    )


def enter(heads, h, g):
    sem = pltpu.get_barrier_semaphore()

    @pl.loop(1, heads)
    def _(i):
        pl.semaphore_signal(
            sem, inc=1, device_id=to_head(lax.rem(h + i, heads)), device_id_type=pl.DeviceIdType.MESH
        )

    for other in (g ^ 1, g ^ 2):
        pl.semaphore_signal(
            sem, inc=1, device_id=to_client(other), device_id_type=pl.DeviceIdType.MESH
        )


def await_others(heads):
    pl.semaphore_wait(pltpu.get_barrier_semaphore(), heads + 1)


def round_kernel(
    heads, steps, ids, token_row, label_row, client_table, in_weight, in_bias, head_weight, byte_table, out_table,
    spread, back_parts, hidden_out, preact_out, chosen_out, loss_out,
    wv, ct, iw, ib, tables, chosen_v, preact_v, hidden_v, s1, r1, k2, s2, r2, s3,
    factors, flat, spaced, b0, gram_ii, gram_io, gram_oo, pair_count, deltas,
    e, x, db, acc, b1s, b1r, tot, b2,
    w_sem, in_sem, out_sem, p_send, p_recv, y_send, y_recv, f_send, f_recv,
    t_own_send, t_own_recv, t_send, t_recv, t_pair_send, t_pair_recv,
    d_send, d_recv, e_send, e_recv, b_send, b_recv, c_send, c_recv, o_sem, z_sem,
):
    h, g = lax.axis_index("head"), lax.axis_index("client")
    core, far = g & 1, g >> 1
    pair, peer = g ^ 1, g ^ 2
    x_side, z_side = h ^ 1, h ^ 2
    clients, units = hidden_v.shape
    group = clients // 4
    each = clients // heads
    block_rows = steps * PIECE_ROWS
    width = PIECE_ROWS * LANES
    vocab = tables.shape[2]
    part = vocab // 4 // (TABLE_PIECES // 2)

    enter(heads, h, g)

    small = [
        pltpu.make_async_copy(client_table, ct, in_sem.at[0]),
        pltpu.make_async_copy(in_weight, iw, in_sem.at[1]),
        pltpu.make_async_copy(in_bias, ib, in_sem.at[2]),
        pltpu.make_async_copy(byte_table, tables.at[0, g], in_sem.at[3]),
        pltpu.make_async_copy(out_table, tables.at[1, g], in_sem.at[4]),
    ]
    for c in small:
        c.start()

    def w_copy(k):
        return pltpu.make_async_copy(
            head_weight.at[:, pl.ds(pl.multiple_of(k * width, width), width)], wv.at[k], w_sem.at[k]
        )

    @pl.loop(0, steps)
    def _(k):
        w_copy(k).start()

    for c in small:
        c.wait()
    population = lax.broadcasted_iota(jnp.int32, (clients, ct.shape[0]), 1)
    onehot = jnp.where(ids[...] == population, 1.0, 0.0).astype(BF16)
    chosen = jnp.dot(onehot, ct[...], preferred_element_type=F32).astype(BF16)
    chosen_v[...] = chosen
    preact = jnp.dot(chosen, iw[...], preferred_element_type=F32) + ib[...]
    preact_v[...] = preact
    hidden_v[...] = jnp.maximum(preact, 0.0).astype(BF16)

    def rows_of(head, k):
        return pl.ds(pl.multiple_of(head * block_rows + k * PIECE_ROWS, PIECE_ROWS), PIECE_ROWS)

    def piece(t, owner_head, col):
        table = lax.div(t, TABLE_PIECES // 2)
        row = lax.rem(owner_head, 4) * (vocab // 4) + lax.rem(t, TABLE_PIECES // 2) * part
        return tables.at[table, col, pl.ds(pl.multiple_of(row, part), part)]

    own_to_pair = [
        remote(tables.at[t, g], tables.at[t, g], t_own_send.at[t], t_own_recv.at[t], to_client(pair))
        for t in range(2)
    ]

    def t_peer(t):
        ref = piece(t, h, g)
        return remote(ref, ref, t_send.at[0, t], t_recv.at[0, t], to_client(peer))

    def t_side(kind, t):
        ref = piece(t, h, peer)
        return remote(ref, ref, t_send.at[kind, t], t_recv.at[kind, t], to_head((x_side, z_side)[kind - 1]))

    def t_relay(t, odd):
        ref = piece(t, x_side if odd else z_side, peer)
        return remote(ref, ref, t_send.at[3, t], t_recv.at[3, t], to_head(z_side if odd else x_side))

    def t_pair(kind, t):
        ref = piece(t, (h, x_side, z_side, h ^ 3)[kind], peer)
        return remote(ref, ref, t_pair_send.at[kind, t], t_pair_recv.at[kind, t], to_client(pair))

    def to_pair(k):
        return remote(
            s1.at[k, pl.ds((1 - core) * 2 * group, 2 * group)], r1.at[k],
            p_send.at[k], p_recv.at[k], to_client(pair),
        )

    def to_peer(k):
        return remote(s2.at[k], r2.at[k], y_send.at[k], y_recv.at[k], to_client(peer))

    def to_owner(k, i):
        other = lax.rem(h + i, heads)
        return remote(
            s3.at[k, other], factors.at[rows_of(h, k)],
            f_send.at[k, other], f_recv.at[k, h], to_head(other),
        )

    def from_holder(k, i):
        other = lax.rem(h + i, heads)
        return remote(
            s3.at[k, other], factors.at[rows_of(other, k)],
            f_send.at[k, other], f_recv.at[k, other], to_head(other),
        )

    small_out = [
        pltpu.make_async_copy(hidden_v, hidden_out, out_sem.at[0]),
        pltpu.make_async_copy(preact_v, preact_out, out_sem.at[1]),
        pltpu.make_async_copy(chosen_v, chosen_out, out_sem.at[2]),
    ]
    for c in small_out:
        c.start()

    def multiply_stage(k):
        w_copy(k).wait()
        for n in range(width // 512):
            out = jnp.dot(
                hidden_v[...], wv[k, :, n * 512 : (n + 1) * 512], preferred_element_type=F32
            )
            for q in range(4):
                s1[k, :, n * 4 + q, :] = out[:, q * LANES : (q + 1) * LANES]

    def pair_stage(k):
        to_pair(k).wait_recv()
        theirs = core * 2 * group + (1 - far) * group
        mine = core * 2 * group + far * group
        s2[k] = (s1[k, pl.ds(theirs, group)] + r1[k, pl.ds((1 - far) * group, group)]).astype(BF16)
        to_peer(k).start()
        k2[k] = s1[k, pl.ds(mine, group)] + r1[k, pl.ds(far * group, group)]

    def peer_stage(k):
        to_peer(k).wait_recv()
        s3[k] = (k2[k] + r2[k].astype(F32)).astype(BF16)

        @pl.loop(1, heads)
        def _(i):
            to_owner(k, i).start()

        factors[rows_of(h, k)] = s3[k, h]

    def table_stage(k):
        for kind, start in ((0, 2), (1, 4), (2, 6)):
            @pl.when((k >= start) & (k < start + TABLE_PIECES // 2))
            def _():
                for odd in (False, True):
                    t = 2 * (k - start) + (1 if odd else 0)
                    if kind == 0:
                        t_peer(t).wait_recv()
                        t_side(1, t).start()
                        t_side(2, t).start()
                        t_pair(0, t).start()
                    elif kind == 1:
                        t_side(1, t).wait_recv()
                        t_side(2, t).wait_recv()
                        t_relay(t, odd).start()
                        t_pair(1, t).start()
                        t_pair(2, t).start()
                    else:
                        t_relay(t, odd).wait_recv()
                        t_pair(3, t).start()

    await_others(heads)

    @pl.loop(0, TABLE_PIECES)
    def _(t):
        t_peer(t).start()

    for c in own_to_pair:
        c.start()

    PEER_LAG = 4

    @pl.loop(0, max(steps + PEER_LAG, TABLE_PIECES // 2 + 6))
    def _(k):
        @pl.when(k < steps)
        def _():
            multiply_stage(k)
            to_pair(k).start()

        @pl.when((k >= 1) & (k < steps + 1))
        def _():
            pair_stage(k - 1)

        @pl.when((k >= PEER_LAG) & (k < steps + PEER_LAG))
        def _():
            peer_stage(k - PEER_LAG)

        table_stage(k)

    for c in own_to_pair:
        c.wait_recv()

    @pl.loop(0, TABLE_PIECES)
    def _(t):
        for kind in range(4):
            t_pair(kind, t).wait_recv()

    gram_ii[...], gram_io[...], gram_oo[...] = table_products(tables)
    pair_count[...] = token_pairs(token_row[...], label_row[...], vocab)

    @pl.loop(0, steps)
    def _(k):
        @pl.loop(1, heads)
        def _(i):
            from_holder(k, i).wait_recv()

    train(factors, flat, spaced, b0, loss_out, deltas, tables, (gram_ii, gram_io, gram_oo), pair_count)

    def place(c):
        return (c & 1) * 2 + (c >> 1)

    def to_holder(k, i):
        other = lax.rem(h + i, heads)
        return remote(
            deltas.at[rows_of(other, k)], e.at[place(g), k, h],
            d_send.at[k, other], d_recv.at[k, h], to_head(other),
        )

    def from_owner(k, i):
        other = lax.rem(h + i, heads)
        return remote(
            deltas.at[rows_of(other, k)], e.at[place(g), k, other],
            d_send.at[k, other], d_recv.at[k, other], to_head(other),
        )

    def group_copy(kind, k, receive):
        sender = (peer, pair, pair)[kind] if receive else g
        ref = e.at[place((sender, sender, sender ^ 2)[kind]), k]
        return remote(ref, ref, e_send.at[kind, k], e_recv.at[kind, k], to_client((peer, pair, pair)[kind]))

    @pl.loop(0, steps)
    def _(k):
        @pl.loop(1, heads)
        def _(i):
            to_holder(k, i).start()

    acc[...] = jnp.zeros_like(acc)

    def spread_out(k):
        return pltpu.make_async_copy(
            db.at[k], spread.at[:, pl.ds(pl.multiple_of(k * width, width), width)], o_sem.at[k]
        )

    @pl.loop(0, steps + 2)
    def _(k):
        @pl.when(k < steps)
        def _():
            e[place(g), k, h] = deltas[rows_of(h, k)]

            @pl.loop(1, heads)
            def _(i):
                from_owner(k, i).wait_recv()

            group_copy(0, k, False).start()
            group_copy(1, k, False).start()

        @pl.when((k >= 1) & (k < steps + 1))
        def _():
            group_copy(0, k - 1, True).wait_recv()
            group_copy(2, k - 1, False).start()

        @pl.when(k >= 2)
        def _():
            j = k - 2
            group_copy(1, j, True).wait_recv()
            group_copy(2, j, True).wait_recv()
            for c in range(4):
                x[c * group : (c + 1) * group] = e[c, j].astype(F32)
            for q in range(PIECE_ROWS):
                db[j, :, q * LANES : (q + 1) * LANES] = x[:, q, :].astype(BF16)
            spread_out(j).start()
            acc[...] += lax.dot_general(
                wv[j], db[j], (((1,), (1,)), ((), ())), preferred_element_type=F32
            )

    turned = acc[...].T
    for j in range(heads):
        for b in range(units // LANES):
            b1s[j, b * each : (b + 1) * each, :] = turned[
                j * each : (j + 1) * each, b * LANES : (b + 1) * LANES
            ]

    def part_to(i):
        other = lax.rem(h + i, heads)
        return remote(b1s.at[other], b1r.at[h], b_send.at[other], b_recv.at[h], to_head(other))

    def part_from(i):
        other = lax.rem(h + i, heads)
        return remote(b1s.at[other], b1r.at[other], b_send.at[other], b_recv.at[other], to_head(other))

    def sum_to(i):
        other = lax.rem(h + i, heads)
        return remote(tot, b2.at[h], c_send.at[other], c_recv.at[h], to_head(other))

    def sum_from(i):
        other = lax.rem(h + i, heads)
        return remote(tot, b2.at[other], c_send.at[other], c_recv.at[other], to_head(other))

    @pl.loop(1, heads)
    def _(i):
        part_to(i).start()

    @pl.loop(0, steps)
    def _(k):
        to_pair(k).wait_send()
        to_peer(k).wait_send()
        spread_out(k).wait()
        for kind in range(3):
            group_copy(kind, k, False).wait_send()

        @pl.loop(1, heads)
        def _(i):
            to_owner(k, i).wait_send()
            to_holder(k, i).wait_send()

    for c in own_to_pair:
        c.wait_send()
    for c in small_out:
        c.wait()

    @pl.loop(0, TABLE_PIECES)
    def _(t):
        t_peer(t).wait_send()
        t_side(1, t).wait_send()
        t_side(2, t).wait_send()
        t_relay(t, False).wait_send()
        for kind in range(4):
            t_pair(kind, t).wait_send()

    tot[...] = b1s[h]

    @pl.loop(1, heads)
    def _(i):
        part_from(i).wait_recv()
        tot[...] += b1r[lax.rem(h + i, heads)]

    @pl.loop(1, heads)
    def _(i):
        sum_to(i).start()

    b2[h] = tot[...]

    @pl.loop(1, heads)
    def _(i):
        part_to(i).wait_send()
        sum_to(i).wait_send()
        sum_from(i).wait_recv()

    last = pltpu.make_async_copy(b2, back_parts, z_sem)
    last.start()
    last.wait()


def grad_kernel(heads, hidden, spread, back_parts, preact, chosen, head_grad, in_grad, turned, hb):
    clients, units = hidden.shape
    each = clients // heads

    @pl.when(pl.program_id(0) == 0)
    def _():
        turned[...] = hidden[...].astype(F32).T.astype(BF16)
        for j in range(heads):
            for b in range(units // LANES):
                hb[j * each : (j + 1) * each, b * LANES : (b + 1) * LANES] = back_parts[
                    j, b * each : (b + 1) * each, :
                ]
        masked = jnp.where(preact[...] > 0, hb[...], 0.0)
        top = masked.astype(BF16)
        rest = masked - top.astype(F32)
        mid = rest.astype(BF16)
        low = (rest - mid.astype(F32)).astype(BF16)
        sel = chosen[...]
        total = jnp.zeros(in_grad.shape, F32)
        for term in (low, mid, top):
            total += lax.dot_general(sel, term, (((0,), (0,)), ((), ())), preferred_element_type=F32)
        in_grad[...] = total

    head_grad[...] = jnp.dot(turned[...], spread[...], preferred_element_type=F32).astype(BF16)


def local(
    client_ids, client_table, in_weight, in_bias, head_weight, tokens, labels, byte_table, out_table
):
    heads = lax.axis_size("head")
    groups = lax.axis_size("client")
    assert groups == 4 and tokens.shape[0] == 1 and heads % 4 == 0
    units, columns = head_weight.shape
    clients = client_ids.shape[0]
    embed = client_table.shape[1]
    vocab, share = byte_table.shape
    depth = share * groups
    width = PIECE_ROWS * LANES
    steps = columns // width
    rows = heads * columns // LANES
    group = clients // groups
    each = clients // heads
    part_rows = each * units // LANES
    any_spec = pl.BlockSpec(memory_space=pl.ANY)
    vmem_spec = pl.BlockSpec(memory_space=pltpu.VMEM)
    dma = pltpu.SemaphoreType.DMA

    ordered = client_ids.reshape(heads, 2, 2).transpose(2, 1, 0).reshape(clients, 1)
    vmem = pltpu.VMEM
    spread, back_parts, hidden, preact, chosen, loss = pl.pallas_call(
        functools.partial(round_kernel, heads, steps),
        name="round",
        out_shape=[
            jax.ShapeDtypeStruct((clients, columns), BF16),
            jax.ShapeDtypeStruct((heads, part_rows, LANES), F32),
            jax.ShapeDtypeStruct((clients, units), BF16),
            jax.ShapeDtypeStruct((clients, units), F32),
            jax.ShapeDtypeStruct((clients, embed), BF16),
            jax.ShapeDtypeStruct((8, LANES), F32),
        ],
        in_specs=[vmem_spec] * 3 + [any_spec] * 6,
        out_specs=[any_spec] * 5 + [vmem_spec],
        scratch_shapes=[
            vmem((steps, units, width), BF16),
            vmem(client_table.shape, BF16),
            vmem(in_weight.shape, BF16),
            vmem((1, units), F32),
            vmem((2, groups, vocab, share), BF16),
            vmem((clients, embed), BF16),
            vmem((clients, units), F32),
            vmem((clients, units), BF16),
            vmem((steps, clients, PIECE_ROWS, LANES), F32),
            vmem((steps, 2 * group, PIECE_ROWS, LANES), F32),
            vmem((steps, group, PIECE_ROWS, LANES), F32),
            vmem((steps, group, PIECE_ROWS, LANES), BF16),
            vmem((steps, group, PIECE_ROWS, LANES), BF16),
            vmem((steps, group, PIECE_ROWS, LANES), BF16),
            vmem((rows, LANES), BF16),
            vmem((rows, LANES), F32),
            vmem((depth, LANES), BF16),
            vmem((rows * LANES // (2 * depth), depth), BF16),
            vmem((vocab, vocab), F32),
            vmem((vocab, vocab), F32),
            vmem((vocab, vocab), F32),
            vmem((vocab, vocab), F32),
            vmem((rows, LANES), BF16),
            vmem((groups, steps, heads, PIECE_ROWS, LANES), BF16),
            vmem((clients, PIECE_ROWS, LANES), F32),
            vmem((steps, clients, width), BF16),
            vmem((units, clients), F32),
            vmem((heads, part_rows, LANES), F32),
            vmem((heads, part_rows, LANES), F32),
            vmem((part_rows, LANES), F32),
            vmem((heads, part_rows, LANES), F32),
            dma((steps,)), dma((5,)), dma((3,)),
            dma((steps,)), dma((steps,)), dma((steps,)), dma((steps,)),
            dma((steps, heads)), dma((steps, heads)),
            dma((2,)), dma((2,)), dma((4, TABLE_PIECES)), dma((4, TABLE_PIECES)),
            dma((4, TABLE_PIECES)), dma((4, TABLE_PIECES)),
            dma((steps, heads)), dma((steps, heads)),
            dma((3, steps)), dma((3, steps)),
            dma((heads,)), dma((heads,)), dma((heads,)), dma((heads,)), dma((steps,)), dma,
        ],
        compiler_params=pltpu.CompilerParams(
            collective_id=0, has_side_effects=True, vmem_limit_bytes=HIGH_VMEM
        ),
    )(
        ordered, tokens, labels, client_table, in_weight, in_bias.reshape(1, units), head_weight,
        byte_table, out_table,
    )

    block = 2048
    fixed = lambda *shape: pl.BlockSpec(shape, lambda i: (0,) * len(shape))
    head_grad, in_grad = pl.pallas_call(
        functools.partial(grad_kernel, heads),
        name="grad",
        grid=(columns // block,),
        out_shape=[
            jax.ShapeDtypeStruct((units, columns), BF16),
            jax.ShapeDtypeStruct((embed, units), F32),
        ],
        in_specs=[
            fixed(clients, units),
            pl.BlockSpec((clients, block), lambda i: (0, i)),
            fixed(heads, part_rows, LANES),
            fixed(clients, units),
            fixed(clients, embed),
        ],
        out_specs=[pl.BlockSpec((units, block), lambda i: (0, i)), fixed(embed, units)],
        scratch_shapes=[pltpu.VMEM((units, clients), BF16), pltpu.VMEM((clients, units), F32)],
        compiler_params=pltpu.CompilerParams(vmem_limit_bytes=HIGH_VMEM),
    )(hidden, spread, back_parts, preact, chosen)
    return head_grad, in_grad, loss[0, :1] / tokens.shape[1]


def solution(mesh):
    placed = (
        P(),
        P(),
        P(None, "client"),
        P("client"),
        P("client", "head"),
        P(("head", "client"), None),
        P(("head", "client"), None),
        P(None, "client"),
        P(None, "client"),
    )
    return jax.shard_map(
        local,
        mesh=mesh,
        in_specs=placed,
        out_specs=(P("client", "head"), P(None, "client"), P(("head", "client"))),
        check_vma=False,
    )
```

```python
import functools

import jax
import jax.numpy as jnp
from jax import lax
from jax.experimental import pallas as pl
from jax.experimental.pallas import tpu as pltpu
from jax.sharding import PartitionSpec as P

EPSILON = 1e-06
learn_rate = 0.1
LANES = 128
TILE = 128
PIECE_ROWS = 16
TABLE_PIECES = 8
HIGH_VMEM = 62 * 1024 * 1024
F32 = jnp.float32
BF16 = jnp.bfloat16


def split(x):
    top = x.astype(BF16)
    return top, (x - top.astype(F32)).astype(BF16)


def mm(x, y, over_x=1, over_y=0):
    (x_top, x_low), (y_top, y_low) = split(x), split(y)
    return (
        exact(x_top, y_low, over_x, over_y)
        + exact(x_low, y_top, over_x, over_y)
        + exact(x_top, y_top, over_x, over_y)
    )


def exact(x, y, over_x, over_y):
    return lax.dot_general(
        x, y, (((over_x,), (over_y,)), ((), ())), preferred_element_type=jnp.float32
    )


def inner_step(u, n_in, m_out, k_bb, gram_io, mean_in, pair_count, depth, scale):
    uk = mm(u, k_bb)
    z = gram_io + scale * mm(u, m_out, 1, 1)
    q = mean_in + jnp.sum(u * (2.0 * scale * n_in + (scale * scale) * uk), -1, keepdims=True) / depth
    r = lax.rsqrt(q + EPSILON)
    kappa = 4.0 / float(depth) ** 0.5
    logits = (kappa * r) * z
    top = jnp.max(logits, -1, keepdims=True)
    raised = jnp.exp(logits - top)
    total = jnp.sum(raised, -1, keepdims=True)
    row_count = jnp.sum(pair_count, -1, keepdims=True)
    loss = jnp.sum(
        row_count * (jnp.log(total) + top) - jnp.sum(pair_count * logits, -1, keepdims=True), 0, keepdims=True
    )
    slope = row_count * (raised / total) - pair_count
    dz = (kappa * r) * slope
    dr = kappa * jnp.sum(slope * z, -1, keepdims=True)
    e = dr * (-1.0 / depth) * (r * r * r)
    gu = scale * (mm(dz, m_out) + e * (n_in + scale * uk))
    w = mm(dz, u, 0, 0)
    x = e * u
    y = mm(u, x, 0, 0)
    return loss, gu, w, x, y


def add_grams(tables, grams, c):
    for ref, left, right in zip(grams, (0, 0, 1), (0, 1, 1)):
        ref[...] += exact(tables[left, c], tables[right, c], 1, 1)


def token_pairs(token_row, label_row, vocab):
    ids = lax.broadcasted_iota(jnp.int32, (vocab, token_row.shape[1]), 0)
    return exact(
        jnp.where(ids == token_row, 1.0, 0.0).astype(BF16),
        jnp.where(ids == label_row, 1.0, 0.0).astype(BF16),
        1,
        1,
    )


def widen(factors, flat, spaced, b0, groups):
    rows = factors.shape[0]
    share = spaced.shape[0] // groups
    rank, depth = b0.shape
    per_row = LANES // rank
    across = depth // LANES
    half = rows // 2
    q = half // groups
    flat[...] = factors[...].astype(F32)
    here = lanes_of_row(q, per_row, rank)
    for c in range(groups):
        wide = jnp.broadcast_to(flat[c * q : (c + 1) * q][:, None, :], (q, per_row, LANES))
        spaced[c * share : (c + 1) * share] = jnp.where(here, wide, 0.0).reshape(share, LANES).astype(BF16)
    for n in range(across):
        b0[:, n * LANES : (n + 1) * LANES] = flat[pl.ds(half + n, rank, stride=across), :].astype(BF16)


def lanes_of_row(q, per_row, rank):
    lane = lax.broadcasted_iota(jnp.int32, (q, per_row, LANES), 2)
    sub = lax.broadcasted_iota(jnp.int32, (q, per_row, LANES), 1)
    return lane // rank == sub


def factor_products(tables, spaced, b0, c):
    share = tables.shape[3]
    here = pl.ds(pl.multiple_of(c * share, share), share)
    return (
        exact(tables[0, c], spaced[here], 1, 0),
        exact(tables[0, c], b0[:, here], 1, 1),
        exact(tables[1, c], b0[:, here], 1, 1),
    )


def train(products, flat, b0, loss_ref, deltas, tables, grams, pair_count):
    gram_ii_ref, gram_io_ref, gram_oo_ref = grams
    groups, vocab, share = tables.shape[1:]
    depth = groups * share
    rank = b0.shape[0]
    per_row = LANES // rank
    across = depth // LANES
    half = flat.shape[0] // 2
    scale = 1.0 / float(depth * rank) ** 0.5
    here = lanes_of_row(half // groups, per_row, rank)
    cols = lambda c: slice(c * share, (c + 1) * share)
    fold = jnp.where(
        lax.broadcasted_iota(jnp.int32, (LANES, rank), 0) % rank
        == lax.broadcasted_iota(jnp.int32, (LANES, rank), 1),
        1.0,
        0.0,
    )
    folded, n0, m0 = products
    gram_ii, gram_io, gram_oo = gram_ii_ref[...], gram_io_ref[...], gram_oo_ref[...]
    diagonal = lax.broadcasted_iota(jnp.int32, (vocab, vocab), 0) == lax.broadcasted_iota(
        jnp.int32, (vocab, vocab), 1
    )
    mean_in = jnp.sum(jnp.where(diagonal, gram_ii, 0.0), -1, keepdims=True) / depth
    rn = lax.rsqrt(mean_in + EPSILON)
    u0 = rn * mm(folded, fold)
    k0 = exact(b0[...], b0[...], 1, 1)
    counts = pair_count[...]
    fixed = (gram_io, mean_in, counts, depth, scale)
    first_loss, gu0, w0, x0, y0 = inner_step(u0, n0, m0, k0, *fixed)
    loss_ref[...] = jnp.broadcast_to(first_loss, loss_ref.shape)
    rate = learn_rate * scale
    w0, x0, y0 = -rate * w0, -rate * x0, (-rate * scale) * y0
    u1 = u0 - learn_rate * rn * mm(gram_ii, rn * gu0)
    n1 = n0 + mm(gram_io, w0) + mm(gram_ii, x0) + mm(n0, y0)
    m1 = m0 + mm(gram_oo, w0) + mm(gram_io, x0, 0, 0) + mm(m0, y0)
    cross = k0 + mm(y0, k0, 0, 0) + mm(w0, m0, 0, 0) + mm(x0, n0, 0, 0)
    k1 = cross + mm(cross, y0) + mm(m1, w0, 0, 0) + mm(n1, x0, 0, 0)
    _, gu1, w1, x1, y1 = inner_step(u1, n1, m1, k1, *fixed)
    w1, x1, y1 = -rate * w1, -rate * x1, (-rate * scale) * y1
    ga = (-learn_rate) * rn * (gu0 + gu1)
    wf = w0 + w1 + mm(w0, y1)
    xf = x0 + x1 + mm(x0, y1)
    yf = y0 + y1 + mm(y0, y1)

    repeat = jnp.where(
        lax.broadcasted_iota(jnp.int32, (rank, LANES), 1) % rank
        == lax.broadcasted_iota(jnp.int32, (rank, LANES), 0),
        1.0,
        0.0,
    ).astype(BF16)
    ga_top, ga_low = (exact(t, repeat, 1, 0).astype(BF16) for t in split(ga))
    for c in range(groups):
        q = half // groups
        wide = exact(tables[0, c], ga_top, 0, 0) + exact(tables[0, c], ga_low, 0, 0)
        flat[c * q : (c + 1) * q] = jnp.sum(
            jnp.where(here, wide.reshape(q, per_row, LANES), 0.0), axis=1
        )
    parts = [jnp.concatenate([t.T for t in split(v)], 0) for v in (wf, xf, yf)]
    for c in range(groups):
        db = (
            exact(parts[0], tables[1, c], 1, 0)
            + exact(parts[1], tables[0, c], 1, 0)
            + exact(parts[2], b0[:, cols(c)], 1, 0)
        )
        db = db[:rank] + db[rank:]
        for n in range(share // LANES):
            flat[pl.ds(half + c * (share // LANES) + n, rank, stride=across), :] = db[
                :, n * LANES : (n + 1) * LANES
            ]
    deltas[...] = flat[...].astype(BF16)


def to_head(h):
    return {"head": h}


def to_client(g):
    return {"client": g}


def remote(src, dst, send, recv, device):
    return pltpu.make_async_remote_copy(
        src_ref=src,
        dst_ref=dst,
        send_sem=send,
        recv_sem=recv,
        device_id=device,
        device_id_type=pl.DeviceIdType.MESH,
    )


def enter(heads, h, g):
    sem = pltpu.get_barrier_semaphore()

    @pl.loop(1, heads)
    def _(i):
        pl.semaphore_signal(
            sem, inc=1, device_id=to_head(lax.rem(h + i, heads)), device_id_type=pl.DeviceIdType.MESH
        )

    for other in (g ^ 1, g ^ 2):
        pl.semaphore_signal(
            sem, inc=1, device_id=to_client(other), device_id_type=pl.DeviceIdType.MESH
        )


def await_others(heads):
    pl.semaphore_wait(pltpu.get_barrier_semaphore(), heads + 1)


def round_kernel(
    heads, steps, ids, token_row, label_row, client_table, in_weight, in_bias, head_weight, byte_table, out_table,
    spread, back_parts, hidden_out, preact_out, chosen_out, loss_out,
    wv, ct, iw, ib, tables, chosen_v, preact_v, hidden_v, s1, r1, k2, s2, r2, s3,
    factors, flat, spaced, b0, gram_ii, gram_io, gram_oo, pair_count, deltas,
    e, x, db, acc, b1s, b1r, tot, b2,
    w_sem, in_sem, out_sem, p_send, p_recv, y_send, y_recv, f_send, f_recv,
    t_own_send, t_own_recv, t_send, t_recv, t_pair_send, t_pair_recv,
    d_send, d_recv, e_send, e_recv, b_send, b_recv, c_send, c_recv, o_sem, z_sem,
):
    h, g = lax.axis_index("head"), lax.axis_index("client")
    core, far = g & 1, g >> 1
    pair, peer = g ^ 1, g ^ 2
    x_side, z_side = h ^ 1, h ^ 2
    clients, units = hidden_v.shape
    group = clients // 4
    each = clients // heads
    block_rows = steps * PIECE_ROWS
    width = PIECE_ROWS * LANES
    vocab = tables.shape[2]
    part = vocab // 4 // (TABLE_PIECES // 2)

    enter(heads, h, g)

    small = [
        pltpu.make_async_copy(client_table, ct, in_sem.at[0]),
        pltpu.make_async_copy(in_weight, iw, in_sem.at[1]),
        pltpu.make_async_copy(in_bias, ib, in_sem.at[2]),
        pltpu.make_async_copy(byte_table, tables.at[0, g], in_sem.at[3]),
        pltpu.make_async_copy(out_table, tables.at[1, g], in_sem.at[4]),
    ]
    for c in small:
        c.start()

    def w_copy(k):
        return pltpu.make_async_copy(
            head_weight.at[:, pl.ds(pl.multiple_of(k * width, width), width)], wv.at[k], w_sem.at[k]
        )

    @pl.loop(0, steps)
    def _(k):
        w_copy(k).start()

    for c in small:
        c.wait()
    population = lax.broadcasted_iota(jnp.int32, (ct.shape[0], clients), 0)
    onehot = jnp.where(population == ids[...][None, :], 1.0, 0.0).astype(BF16)
    in_order = exact(onehot, ct[...], 0, 0).astype(BF16)
    row = lax.broadcasted_iota(jnp.int32, (clients, clients), 0)
    slot = lax.broadcasted_iota(jnp.int32, (clients, clients), 1)
    slot_of_row = row % heads * 4 + row // heads % 2 * 2 + row // heads // 2
    chosen = exact(jnp.where(slot == slot_of_row, 1.0, 0.0).astype(BF16), in_order, 1, 0).astype(BF16)
    chosen_v[...] = chosen
    preact = jnp.dot(chosen, iw[...], preferred_element_type=F32) + ib[...][None, :]
    preact_v[...] = preact
    hidden_v[...] = jnp.maximum(preact, 0.0).astype(BF16)

    def rows_of(head, k):
        return pl.ds(pl.multiple_of(head * block_rows + k * PIECE_ROWS, PIECE_ROWS), PIECE_ROWS)

    def piece(t, owner_head, col):
        table = lax.div(t, TABLE_PIECES // 2)
        row = lax.rem(owner_head, 4) * (vocab // 4) + lax.rem(t, TABLE_PIECES // 2) * part
        return tables.at[table, col, pl.ds(pl.multiple_of(row, part), part)]

    own_to_pair = [
        remote(tables.at[t, g], tables.at[t, g], t_own_send.at[t], t_own_recv.at[t], to_client(pair))
        for t in range(2)
    ]

    def t_peer(t):
        ref = piece(t, h, g)
        return remote(ref, ref, t_send.at[0, t], t_recv.at[0, t], to_client(peer))

    def t_side(kind, t):
        ref = piece(t, h, peer)
        return remote(ref, ref, t_send.at[kind, t], t_recv.at[kind, t], to_head((x_side, z_side)[kind - 1]))

    def t_relay(t, odd):
        ref = piece(t, x_side if odd else z_side, peer)
        return remote(ref, ref, t_send.at[3, t], t_recv.at[3, t], to_head(z_side if odd else x_side))

    def t_pair(kind, t):
        ref = piece(t, (h, x_side, z_side, h ^ 3)[kind], peer)
        return remote(ref, ref, t_pair_send.at[kind, t], t_pair_recv.at[kind, t], to_client(pair))

    def to_pair(k):
        return remote(
            s1.at[k, pl.ds((1 - core) * 2 * group, 2 * group)], r1.at[k],
            p_send.at[k], p_recv.at[k], to_client(pair),
        )

    def to_peer(k):
        return remote(s2.at[k], r2.at[k], y_send.at[k], y_recv.at[k], to_client(peer))

    def to_owner(k, i):
        other = lax.rem(h + i, heads)
        return remote(
            s3.at[k, other], factors.at[rows_of(h, k)],
            f_send.at[k, other], f_recv.at[k, h], to_head(other),
        )

    def from_holder(k, i):
        other = lax.rem(h + i, heads)
        return remote(
            s3.at[k, other], factors.at[rows_of(other, k)],
            f_send.at[k, other], f_recv.at[k, other], to_head(other),
        )

    small_out = [
        pltpu.make_async_copy(hidden_v, hidden_out, out_sem.at[0]),
        pltpu.make_async_copy(preact_v, preact_out, out_sem.at[1]),
        pltpu.make_async_copy(chosen_v, chosen_out, out_sem.at[2]),
    ]
    for c in small_out:
        c.start()

    def multiply_stage(k):
        w_copy(k).wait()
        for n in range(width // 512):
            out = jnp.dot(
                hidden_v[...], wv[k, :, n * 512 : (n + 1) * 512], preferred_element_type=F32
            )
            for q in range(4):
                s1[k, :, n * 4 + q, :] = out[:, q * LANES : (q + 1) * LANES]

    def pair_stage(k):
        to_pair(k).wait_recv()
        theirs = core * 2 * group + (1 - far) * group
        mine = core * 2 * group + far * group
        s2[k] = (s1[k, pl.ds(theirs, group)] + r1[k, pl.ds((1 - far) * group, group)]).astype(BF16)
        to_peer(k).start()
        k2[k] = s1[k, pl.ds(mine, group)] + r1[k, pl.ds(far * group, group)]

    def peer_stage(k):
        to_peer(k).wait_recv()
        s3[k] = (k2[k] + r2[k].astype(F32)).astype(BF16)

        @pl.loop(1, heads)
        def _(i):
            to_owner(k, i).start()

        factors[rows_of(h, k)] = s3[k, h]

    def table_stage(k):
        for kind, start in ((0, 2), (1, 4), (2, 6)):
            @pl.when((k >= start) & (k < start + TABLE_PIECES // 2))
            def _():
                for odd in (False, True):
                    t = 2 * (k - start) + (1 if odd else 0)
                    if kind == 0:
                        t_peer(t).wait_recv()
                        t_side(1, t).start()
                        t_side(2, t).start()
                        t_pair(0, t).start()
                    elif kind == 1:
                        t_side(1, t).wait_recv()
                        t_side(2, t).wait_recv()
                        t_relay(t, odd).start()
                        t_pair(1, t).start()
                        t_pair(2, t).start()
                    else:
                        t_relay(t, odd).wait_recv()
                        t_pair(3, t).start()

    grams = (gram_ii, gram_io, gram_oo)
    for ref in grams:
        ref[...] = jnp.zeros_like(ref)
    pair_count[...] = token_pairs(token_row[...], label_row[...], vocab)
    await_others(heads)

    @pl.loop(0, TABLE_PIECES)
    def _(t):
        t_peer(t).start()

    for c in own_to_pair:
        c.start()

    PEER_LAG = 6

    @pl.loop(0, max(steps + PEER_LAG, TABLE_PIECES // 2 + 6))
    def _(k):
        @pl.when(k < steps)
        def _():
            multiply_stage(k)
            to_pair(k).start()

        @pl.when((k >= 1) & (k < steps + 1))
        def _():
            pair_stage(k - 1)

        @pl.when((k >= PEER_LAG) & (k < steps + PEER_LAG))
        def _():
            peer_stage(k - PEER_LAG)

        @pl.when(k == steps)
        def _():
            for c in own_to_pair:
                c.wait_recv()

            @pl.loop(0, 2)
            def _(i):
                add_grams(tables, grams, g ^ i)

        table_stage(k)

    @pl.loop(0, steps)
    def _(k):
        @pl.loop(1, heads)
        def _(i):
            from_holder(k, i).wait_recv()

    widen(factors, flat, spaced, b0, 4)
    near = [factor_products(tables, spaced, b0, c) for c in (g, pair)]
    add_grams(tables, grams, peer)
    near.append(factor_products(tables, spaced, b0, peer))

    @pl.loop(0, TABLE_PIECES)
    def _(t):
        for kind in range(4):
            t_pair(kind, t).wait_recv()

    add_grams(tables, grams, g ^ 3)
    near.append(factor_products(tables, spaced, b0, g ^ 3))
    products = [a + b + c + d for a, b, c, d in zip(*near)]
    train(products, flat, b0, loss_out, deltas, tables, grams, pair_count)

    def place(c):
        return (c & 1) * 2 + (c >> 1)

    def to_holder(k, i):
        other = lax.rem(h + i, heads)
        return remote(
            deltas.at[rows_of(other, k)], e.at[place(g), k, h],
            d_send.at[k, other], d_recv.at[k, h], to_head(other),
        )

    def from_owner(k, i):
        other = lax.rem(h + i, heads)
        return remote(
            deltas.at[rows_of(other, k)], e.at[place(g), k, other],
            d_send.at[k, other], d_recv.at[k, other], to_head(other),
        )

    def group_copy(kind, k, receive):
        sender = (peer, pair, pair)[kind] if receive else g
        ref = e.at[place((sender, sender, sender ^ 2)[kind]), k]
        return remote(ref, ref, e_send.at[kind, k], e_recv.at[kind, k], to_client((peer, pair, pair)[kind]))

    @pl.loop(0, steps)
    def _(k):
        @pl.loop(1, heads)
        def _(i):
            to_holder(k, i).start()

    acc[...] = jnp.zeros_like(acc)

    def spread_out(k):
        return pltpu.make_async_copy(
            db.at[k], spread.at[:, pl.ds(pl.multiple_of(k * width, width), width)], o_sem.at[k]
        )

    PEER_AFTER, PAIR_AFTER = 3, 5

    @pl.loop(0, steps + PAIR_AFTER)
    def _(k):
        @pl.when(k < steps)
        def _():
            e[place(g), k, h] = deltas[rows_of(h, k)]

            @pl.loop(1, heads)
            def _(i):
                from_owner(k, i).wait_recv()

            group_copy(0, k, False).start()
            group_copy(1, k, False).start()

        @pl.when((k >= PEER_AFTER) & (k < steps + PEER_AFTER))
        def _():
            group_copy(0, k - PEER_AFTER, True).wait_recv()
            group_copy(2, k - PEER_AFTER, False).start()

        @pl.when(k >= PAIR_AFTER)
        def _():
            j = k - PAIR_AFTER
            group_copy(1, j, True).wait_recv()
            group_copy(2, j, True).wait_recv()
            apart = clients + 4
            for c in range(4):
                for i in range(group):
                    x[pl.ds(c * group + i, PIECE_ROWS, stride=apart), :] = e[c, j, i].astype(F32)
            for q in range(PIECE_ROWS):
                db[j, :, q * LANES : (q + 1) * LANES] = x[q * apart : q * apart + clients, :].astype(BF16)
            spread_out(j).start()
            acc[...] += lax.dot_general(
                wv[j], db[j], (((1,), (1,)), ((), ())), preferred_element_type=F32
            )

    turned = acc[...].T
    for j in range(heads):
        for b in range(units // LANES):
            b1s[j, b * each : (b + 1) * each, :] = turned[
                j * each : (j + 1) * each, b * LANES : (b + 1) * LANES
            ]

    def part_to(i):
        other = lax.rem(h + i, heads)
        return remote(b1s.at[other], b1r.at[h], b_send.at[other], b_recv.at[h], to_head(other))

    def part_from(i):
        other = lax.rem(h + i, heads)
        return remote(b1s.at[other], b1r.at[other], b_send.at[other], b_recv.at[other], to_head(other))

    def sum_to(i):
        other = lax.rem(h + i, heads)
        return remote(tot, b2.at[h], c_send.at[other], c_recv.at[h], to_head(other))

    def sum_from(i):
        other = lax.rem(h + i, heads)
        return remote(tot, b2.at[other], c_send.at[other], c_recv.at[other], to_head(other))

    @pl.loop(1, heads)
    def _(i):
        part_to(i).start()

    @pl.loop(0, steps)
    def _(k):
        to_pair(k).wait_send()
        to_peer(k).wait_send()
        spread_out(k).wait()
        for kind in range(3):
            group_copy(kind, k, False).wait_send()

        @pl.loop(1, heads)
        def _(i):
            to_owner(k, i).wait_send()
            to_holder(k, i).wait_send()

    for c in own_to_pair:
        c.wait_send()
    for c in small_out:
        c.wait()

    @pl.loop(0, TABLE_PIECES)
    def _(t):
        t_peer(t).wait_send()
        t_side(1, t).wait_send()
        t_side(2, t).wait_send()
        t_relay(t, False).wait_send()
        for kind in range(4):
            t_pair(kind, t).wait_send()

    tot[...] = b1s[h]

    @pl.loop(1, heads)
    def _(i):
        part_from(i).wait_recv()
        tot[...] += b1r[lax.rem(h + i, heads)]

    @pl.loop(1, heads)
    def _(i):
        sum_to(i).start()

    b2[h] = tot[...]

    @pl.loop(1, heads)
    def _(i):
        part_to(i).wait_send()
        sum_to(i).wait_send()
        sum_from(i).wait_recv()

    last = pltpu.make_async_copy(b2, back_parts, z_sem)
    last.start()
    last.wait()


def grad_kernel(
    heads, tokens, hidden, spread, back_parts, preact, chosen, loss,
    head_grad, in_grad, losses, turned, hb, stage, ig, g_sem, i_sem,
):
    clients, units = hidden.shape
    each = clients // heads
    slots, _, block = stage.shape
    steps = spread.shape[1] // block
    turned[...] = hidden[...].astype(F32).T.astype(BF16)

    def block_out(k):
        return pltpu.make_async_copy(
            stage.at[lax.rem(k, slots)],
            head_grad.at[:, pl.ds(pl.multiple_of(k * block, block), block)],
            g_sem.at[lax.rem(k, slots)],
        )

    def fill(first, last):
        @pl.loop(first, last)
        def _(k):
            @pl.when(k >= slots)
            def _():
                block_out(k - slots).wait()

            part = spread[:, pl.ds(pl.multiple_of(k * block, block), block)]
            for m in range(0, units, TILE):
                for n in range(0, block, 2 * TILE):
                    stage[lax.rem(k, slots), m : m + TILE, n : n + 2 * TILE] = jnp.dot(
                        turned[m : m + TILE], part[:, n : n + 2 * TILE], preferred_element_type=F32
                    ).astype(BF16)
            block_out(k).start()

    early = min(slots, steps)
    fill(0, early)
    losses[0] = jnp.max(loss[...]) * (1.0 / tokens)
    for j in range(heads):
        for b in range(units // LANES):
            hb[j * each : (j + 1) * each, b * LANES : (b + 1) * LANES] = back_parts[
                j, b * each : (b + 1) * each, :
            ]
    masked = jnp.where(preact[...] > 0, hb[...], 0.0)
    top = masked.astype(BF16)
    rest = masked - top.astype(F32)
    mid = rest.astype(BF16)
    low = (rest - mid.astype(F32)).astype(BF16)
    sel = chosen[...]
    total = jnp.zeros(ig.shape, F32)
    for term in (low, mid, top):
        total += lax.dot_general(sel, term, (((0,), (0,)), ((), ())), preferred_element_type=F32)
    ig[...] = total
    ig_out = pltpu.make_async_copy(ig, in_grad, i_sem)
    ig_out.start()
    fill(early, steps)

    @pl.loop(steps - early, steps)
    def _(k):
        block_out(k).wait()

    ig_out.wait()


def local(
    client_ids, client_table, in_weight, in_bias, head_weight, tokens, labels, byte_table, out_table
):
    heads = lax.axis_size("head")
    groups = lax.axis_size("client")
    assert groups == 4 and tokens.shape[0] == 1 and heads % 4 == 0
    units, columns = head_weight.shape
    clients = client_ids.shape[0]
    embed = client_table.shape[1]
    vocab, share = byte_table.shape
    depth = share * groups
    width = PIECE_ROWS * LANES
    steps = columns // width
    rows = heads * columns // LANES
    group = clients // groups
    each = clients // heads
    part_rows = each * units // LANES
    any_spec = pl.BlockSpec(memory_space=pl.ANY)
    vmem_spec = pl.BlockSpec(memory_space=pltpu.VMEM)
    dma = pltpu.SemaphoreType.DMA

    vmem = pltpu.VMEM
    spread, back_parts, hidden, preact, chosen, loss = pl.pallas_call(
        functools.partial(round_kernel, heads, steps),
        name="round",
        out_shape=[
            jax.ShapeDtypeStruct((clients, columns), BF16),
            jax.ShapeDtypeStruct((heads, part_rows, LANES), F32),
            jax.ShapeDtypeStruct((clients, units), BF16),
            jax.ShapeDtypeStruct((clients, units), F32),
            jax.ShapeDtypeStruct((clients, embed), BF16),
            jax.ShapeDtypeStruct((8, LANES), F32),
        ],
        in_specs=[vmem_spec] * 3 + [any_spec] * 6,
        out_specs=[any_spec] * 5 + [vmem_spec],
        scratch_shapes=[
            vmem((steps, units, width), BF16),
            vmem(client_table.shape, BF16),
            vmem(in_weight.shape, BF16),
            vmem((units,), F32),
            vmem((2, groups, vocab, share), BF16),
            vmem((clients, embed), BF16),
            vmem((clients, units), F32),
            vmem((clients, units), BF16),
            vmem((steps, clients, PIECE_ROWS, LANES), F32),
            vmem((steps, 2 * group, PIECE_ROWS, LANES), F32),
            vmem((steps, group, PIECE_ROWS, LANES), F32),
            vmem((steps, group, PIECE_ROWS, LANES), BF16),
            vmem((steps, group, PIECE_ROWS, LANES), BF16),
            vmem((steps, group, PIECE_ROWS, LANES), BF16),
            vmem((rows, LANES), BF16),
            vmem((rows, LANES), F32),
            vmem((depth, LANES), BF16),
            vmem((rows * LANES // (2 * depth), depth), BF16),
            vmem((vocab, vocab), F32),
            vmem((vocab, vocab), F32),
            vmem((vocab, vocab), F32),
            vmem((vocab, vocab), F32),
            vmem((rows, LANES), BF16),
            vmem((groups, steps, heads, PIECE_ROWS, LANES), BF16),
            vmem((PIECE_ROWS * (clients + 4), LANES), F32),
            vmem((steps, clients, width), BF16),
            vmem((units, clients), F32),
            vmem((heads, part_rows, LANES), F32),
            vmem((heads, part_rows, LANES), F32),
            vmem((part_rows, LANES), F32),
            vmem((heads, part_rows, LANES), F32),
            dma((steps,)), dma((5,)), dma((3,)),
            dma((steps,)), dma((steps,)), dma((steps,)), dma((steps,)),
            dma((steps, heads)), dma((steps, heads)),
            dma((2,)), dma((2,)), dma((4, TABLE_PIECES)), dma((4, TABLE_PIECES)),
            dma((4, TABLE_PIECES)), dma((4, TABLE_PIECES)),
            dma((steps, heads)), dma((steps, heads)),
            dma((3, steps)), dma((3, steps)),
            dma((heads,)), dma((heads,)), dma((heads,)), dma((heads,)), dma((steps,)), dma,
        ],
        compiler_params=pltpu.CompilerParams(
            collective_id=0, has_side_effects=True, vmem_limit_bytes=HIGH_VMEM
        ),
    )(
        client_ids, tokens, labels, client_table, in_weight, in_bias, head_weight,
        byte_table, out_table,
    )

    block = min(1024, columns)
    slots = 4
    head_grad, in_grad, losses = pl.pallas_call(
        functools.partial(grad_kernel, heads, tokens.shape[1]),
        name="grad",
        out_shape=[
            jax.ShapeDtypeStruct((units, columns), BF16),
            jax.ShapeDtypeStruct((embed, units), F32),
            jax.ShapeDtypeStruct((1,), F32),
        ],
        in_specs=[vmem_spec] * 6,
        out_specs=[any_spec, any_spec, pl.BlockSpec(memory_space=pltpu.SMEM)],
        scratch_shapes=[
            vmem((units, clients), BF16),
            vmem((clients, units), F32),
            vmem((slots, units, block), BF16),
            vmem((embed, units), F32),
            dma((slots,)),
            dma,
        ],
        compiler_params=pltpu.CompilerParams(vmem_limit_bytes=HIGH_VMEM),
    )(hidden, spread, back_parts, preact, chosen, loss)
    return head_grad, in_grad, losses


def solution(mesh):
    placed = (
        P(),
        P(),
        P(None, "client"),
        P("client"),
        P("client", "head"),
        P(("head", "client"), None),
        P(("head", "client"), None),
        P(None, "client"),
        P(None, "client"),
    )
    return jax.shard_map(
        local,
        mesh=mesh,
        in_specs=placed,
        out_specs=(P("client", "head"), P(None, "client"), P(("head", "client"))),
        check_vma=False,
    )
```

```python
import functools

import jax
import jax.numpy as jnp
from jax import lax
from jax.experimental import pallas as pl
from jax.experimental.pallas import tpu as pltpu
from jax.sharding import PartitionSpec as P

EPSILON = 1e-06
learn_rate = 0.1
LANES = 128
TILE = 128
PIECE_ROWS = 16
TABLE_PIECES = 8
HIGH_VMEM = 62 * 1024 * 1024
F32 = jnp.float32
BF16 = jnp.bfloat16


def split(x):
    top = x.astype(BF16)
    return top, (x - top.astype(F32)).astype(BF16)


def mm(x, y, over_x=1, over_y=0):
    (x_top, x_low), (y_top, y_low) = split(x), split(y)
    return (
        exact(x_top, y_low, over_x, over_y)
        + exact(x_low, y_top, over_x, over_y)
        + exact(x_top, y_top, over_x, over_y)
    )


def exact(x, y, over_x, over_y):
    return lax.dot_general(
        x, y, (((over_x,), (over_y,)), ((), ())), preferred_element_type=jnp.float32
    )


def inner_step(u, n_in, m_out, k_bb, gram_io, mean_in, pair_count, depth, scale):
    uk = mm(u, k_bb)
    z = gram_io + scale * mm(u, m_out, 1, 1)
    q = mean_in + jnp.sum(u * (2.0 * scale * n_in + (scale * scale) * uk), -1, keepdims=True) / depth
    r = lax.rsqrt(q + EPSILON)
    kappa = 4.0 / float(depth) ** 0.5
    logits = (kappa * r) * z
    top = jnp.max(logits, -1, keepdims=True)
    raised = jnp.exp(logits - top)
    total = jnp.sum(raised, -1, keepdims=True)
    row_count = jnp.sum(pair_count, -1, keepdims=True)
    loss = jnp.sum(
        row_count * (jnp.log(total) + top) - jnp.sum(pair_count * logits, -1, keepdims=True), 0, keepdims=True
    )
    slope = row_count * (raised / total) - pair_count
    dz = (kappa * r) * slope
    dr = kappa * jnp.sum(slope * z, -1, keepdims=True)
    e = dr * (-1.0 / depth) * (r * r * r)
    gu = scale * (mm(dz, m_out) + e * (n_in + scale * uk))
    w = mm(dz, u, 0, 0)
    x = e * u
    y = mm(u, x, 0, 0)
    return loss, gu, w, x, y


def add_grams(tables, grams, c):
    for ref, left, right in zip(grams, (0, 0, 1), (0, 1, 1)):
        ref[...] += exact(tables[left, c], tables[right, c], 1, 1)


def token_pairs(token_row, label_row, vocab):
    ids = lax.broadcasted_iota(jnp.int32, (vocab, token_row.shape[1]), 0)
    return exact(
        jnp.where(ids == token_row, 1.0, 0.0).astype(BF16),
        jnp.where(ids == label_row, 1.0, 0.0).astype(BF16),
        1,
        1,
    )


def widen(factors, flat, spaced, b0, groups):
    rows = factors.shape[0]
    share = spaced.shape[0] // groups
    rank, depth = b0.shape
    per_row = LANES // rank
    across = depth // LANES
    half = rows // 2
    q = half // groups
    flat[...] = factors[...].astype(F32)
    here = lanes_of_row(q, per_row, rank)
    for c in range(groups):
        wide = jnp.broadcast_to(flat[c * q : (c + 1) * q][:, None, :], (q, per_row, LANES))
        spaced[c * share : (c + 1) * share] = jnp.where(here, wide, 0.0).reshape(share, LANES).astype(BF16)
    for n in range(across):
        b0[:, n * LANES : (n + 1) * LANES] = flat[pl.ds(half + n, rank, stride=across), :].astype(BF16)


def lanes_of_row(q, per_row, rank):
    lane = lax.broadcasted_iota(jnp.int32, (q, per_row, LANES), 2)
    sub = lax.broadcasted_iota(jnp.int32, (q, per_row, LANES), 1)
    return lane // rank == sub


def factor_products(tables, spaced, b0, c):
    share = tables.shape[3]
    here = pl.ds(pl.multiple_of(c * share, share), share)
    return (
        exact(tables[0, c], spaced[here], 1, 0),
        exact(tables[0, c], b0[:, here], 1, 1),
        exact(tables[1, c], b0[:, here], 1, 1),
    )


def train(products, flat, b0, loss_ref, deltas, tables, grams, pair_count):
    gram_ii_ref, gram_io_ref, gram_oo_ref = grams
    groups, vocab, share = tables.shape[1:]
    depth = groups * share
    rank = b0.shape[0]
    per_row = LANES // rank
    across = depth // LANES
    half = flat.shape[0] // 2
    scale = 1.0 / float(depth * rank) ** 0.5
    here = lanes_of_row(half // groups, per_row, rank)
    cols = lambda c: slice(c * share, (c + 1) * share)
    fold = jnp.where(
        lax.broadcasted_iota(jnp.int32, (LANES, rank), 0) % rank
        == lax.broadcasted_iota(jnp.int32, (LANES, rank), 1),
        1.0,
        0.0,
    )
    folded, n0, m0 = products
    gram_ii, gram_io, gram_oo = gram_ii_ref[...], gram_io_ref[...], gram_oo_ref[...]
    diagonal = lax.broadcasted_iota(jnp.int32, (vocab, vocab), 0) == lax.broadcasted_iota(
        jnp.int32, (vocab, vocab), 1
    )
    mean_in = jnp.sum(jnp.where(diagonal, gram_ii, 0.0), -1, keepdims=True) / depth
    rn = lax.rsqrt(mean_in + EPSILON)
    u0 = rn * mm(folded, fold)
    k0 = exact(b0[...], b0[...], 1, 1)
    counts = pair_count[...]
    fixed = (gram_io, mean_in, counts, depth, scale)
    first_loss, gu0, w0, x0, y0 = inner_step(u0, n0, m0, k0, *fixed)
    loss_ref[...] = jnp.broadcast_to(first_loss, loss_ref.shape)
    rate = learn_rate * scale
    w0, x0, y0 = -rate * w0, -rate * x0, (-rate * scale) * y0
    u1 = u0 - learn_rate * rn * mm(gram_ii, rn * gu0)
    n1 = n0 + mm(gram_io, w0) + mm(gram_ii, x0) + mm(n0, y0)
    m1 = m0 + mm(gram_oo, w0) + mm(gram_io, x0, 0, 0) + mm(m0, y0)
    cross = k0 + mm(y0, k0, 0, 0) + mm(w0, m0, 0, 0) + mm(x0, n0, 0, 0)
    k1 = cross + mm(cross, y0) + mm(m1, w0, 0, 0) + mm(n1, x0, 0, 0)
    _, gu1, w1, x1, y1 = inner_step(u1, n1, m1, k1, *fixed)
    w1, x1, y1 = -rate * w1, -rate * x1, (-rate * scale) * y1
    ga = (-learn_rate) * rn * (gu0 + gu1)
    wf = w0 + w1 + mm(w0, y1)
    xf = x0 + x1 + mm(x0, y1)
    yf = y0 + y1 + mm(y0, y1)

    repeat = jnp.where(
        lax.broadcasted_iota(jnp.int32, (rank, LANES), 1) % rank
        == lax.broadcasted_iota(jnp.int32, (rank, LANES), 0),
        1.0,
        0.0,
    ).astype(BF16)
    ga_top, ga_low = (exact(t, repeat, 1, 0).astype(BF16) for t in split(ga))
    for c in range(groups):
        q = half // groups
        wide = exact(tables[0, c], ga_top, 0, 0) + exact(tables[0, c], ga_low, 0, 0)
        flat[c * q : (c + 1) * q] = jnp.sum(
            jnp.where(here, wide.reshape(q, per_row, LANES), 0.0), axis=1
        )
    parts = [jnp.concatenate([t.T for t in split(v)], 0) for v in (wf, xf, yf)]
    for c in range(groups):
        db = (
            exact(parts[0], tables[1, c], 1, 0)
            + exact(parts[1], tables[0, c], 1, 0)
            + exact(parts[2], b0[:, cols(c)], 1, 0)
        )
        db = db[:rank] + db[rank:]
        for n in range(share // LANES):
            flat[pl.ds(half + c * (share // LANES) + n, rank, stride=across), :] = db[
                :, n * LANES : (n + 1) * LANES
            ]
    deltas[...] = flat[...].astype(BF16)


def to_head(h):
    return {"head": h}


def to_client(g):
    return {"client": g}


def remote(src, dst, send, recv, device):
    return pltpu.make_async_remote_copy(
        src_ref=src,
        dst_ref=dst,
        send_sem=send,
        recv_sem=recv,
        device_id=device,
        device_id_type=pl.DeviceIdType.MESH,
    )


def enter(heads, h, g):
    sem = pltpu.get_barrier_semaphore()

    @pl.loop(1, heads)
    def _(i):
        pl.semaphore_signal(
            sem, inc=1, device_id=to_head(lax.rem(h + i, heads)), device_id_type=pl.DeviceIdType.MESH
        )

    for other in (g ^ 1, g ^ 2):
        pl.semaphore_signal(
            sem, inc=1, device_id=to_client(other), device_id_type=pl.DeviceIdType.MESH
        )


def await_others(heads):
    pl.semaphore_wait(pltpu.get_barrier_semaphore(), heads + 1)


def round_kernel(
    heads, steps, ids, token_row, label_row, client_table, in_weight, in_bias, head_weight, byte_table, out_table,
    spread, back_parts, hidden_out, preact_out, chosen_out, loss_out,
    wv, ct, iw, ib, tables, chosen_v, preact_v, hidden_v, s1, r1, k2, s2, r2, s3,
    factors, flat, spaced, b0, gram_ii, gram_io, gram_oo, pair_count, deltas,
    e, x, db, acc, b1s, b1r, tot, b2,
    w_sem, in_sem, out_sem, p_send, p_recv, y_send, y_recv, f_send, f_recv,
    t_own_send, t_own_recv, t_send, t_recv, t_pair_send, t_pair_recv,
    d_send, d_recv, e_send, e_recv, b_send, b_recv, c_send, c_recv, o_sem, z_sem,
):
    h, g = lax.axis_index("head"), lax.axis_index("client")
    core, far = g & 1, g >> 1
    pair, peer = g ^ 1, g ^ 2
    x_side, z_side = h ^ 1, h ^ 2
    clients, units = hidden_v.shape
    group = clients // 4
    each = clients // heads
    block_rows = steps * PIECE_ROWS
    width = PIECE_ROWS * LANES
    vocab = tables.shape[2]
    part = vocab // 4 // (TABLE_PIECES // 2)

    enter(heads, h, g)

    small = [
        pltpu.make_async_copy(client_table, ct, in_sem.at[0]),
        pltpu.make_async_copy(in_weight, iw, in_sem.at[1]),
        pltpu.make_async_copy(in_bias, ib, in_sem.at[2]),
        pltpu.make_async_copy(byte_table, tables.at[0, g], in_sem.at[3]),
        pltpu.make_async_copy(out_table, tables.at[1, g], in_sem.at[4]),
    ]
    for c in small:
        c.start()

    def w_copy(k):
        return pltpu.make_async_copy(
            head_weight.at[:, pl.ds(pl.multiple_of(k * width, width), width)], wv.at[k], w_sem.at[k]
        )

    @pl.loop(0, steps)
    def _(k):
        w_copy(k).start()

    for c in small:
        c.wait()
    population = lax.broadcasted_iota(jnp.int32, (ct.shape[0], clients), 0)
    onehot = jnp.where(population == ids[...][None, :], 1.0, 0.0).astype(BF16)
    in_order = exact(onehot, ct[...], 0, 0).astype(BF16)
    row = lax.broadcasted_iota(jnp.int32, (clients, clients), 0)
    slot = lax.broadcasted_iota(jnp.int32, (clients, clients), 1)
    slot_of_row = row % heads * 4 + row // heads % 2 * 2 + row // heads // 2
    chosen = exact(jnp.where(slot == slot_of_row, 1.0, 0.0).astype(BF16), in_order, 1, 0).astype(BF16)
    chosen_v[...] = chosen
    preact = jnp.dot(chosen, iw[...], preferred_element_type=F32) + ib[...][None, :]
    preact_v[...] = preact
    hidden_v[...] = jnp.maximum(preact, 0.0).astype(BF16)

    def rows_of(head, k):
        return pl.ds(pl.multiple_of(head * block_rows + k * PIECE_ROWS, PIECE_ROWS), PIECE_ROWS)

    def piece(t, owner_head, col):
        table = lax.div(t, TABLE_PIECES // 2)
        row = lax.rem(owner_head, 4) * (vocab // 4) + lax.rem(t, TABLE_PIECES // 2) * part
        return tables.at[table, col, pl.ds(pl.multiple_of(row, part), part)]

    own_to_pair = [
        remote(tables.at[t, g], tables.at[t, g], t_own_send.at[t], t_own_recv.at[t], to_client(pair))
        for t in range(2)
    ]

    def t_peer(t):
        ref = piece(t, h, g)
        return remote(ref, ref, t_send.at[0, t], t_recv.at[0, t], to_client(peer))

    def t_side(kind, t):
        ref = piece(t, h, peer)
        return remote(ref, ref, t_send.at[kind, t], t_recv.at[kind, t], to_head((x_side, z_side)[kind - 1]))

    def t_relay(t, odd):
        ref = piece(t, x_side if odd else z_side, peer)
        return remote(ref, ref, t_send.at[3, t], t_recv.at[3, t], to_head(z_side if odd else x_side))

    def t_pair(kind, t):
        ref = piece(t, (h, x_side, z_side, h ^ 3)[kind], peer)
        return remote(ref, ref, t_pair_send.at[kind, t], t_pair_recv.at[kind, t], to_client(pair))

    def to_pair(k):
        return remote(
            s1.at[k, pl.ds((1 - core) * 2 * group, 2 * group)], r1.at[k],
            p_send.at[k], p_recv.at[k], to_client(pair),
        )

    def to_peer(k):
        return remote(s2.at[k], r2.at[k], y_send.at[k], y_recv.at[k], to_client(peer))

    def to_owner(k, i):
        other = lax.rem(h + i, heads)
        return remote(
            s3.at[k, other], factors.at[rows_of(h, k)],
            f_send.at[k, other], f_recv.at[k, h], to_head(other),
        )

    def from_holder(k, i):
        other = lax.rem(h + i, heads)
        return remote(
            s3.at[k, other], factors.at[rows_of(other, k)],
            f_send.at[k, other], f_recv.at[k, other], to_head(other),
        )

    small_out = [
        pltpu.make_async_copy(hidden_v, hidden_out, out_sem.at[0]),
        pltpu.make_async_copy(preact_v, preact_out, out_sem.at[1]),
        pltpu.make_async_copy(chosen_v, chosen_out, out_sem.at[2]),
    ]
    for c in small_out:
        c.start()

    def multiply_stage(k):
        w_copy(k).wait()
        for n in range(width // 512):
            out = jnp.dot(
                hidden_v[...], wv[k, :, n * 512 : (n + 1) * 512], preferred_element_type=F32
            )
            for q in range(4):
                s1[k, :, n * 4 + q, :] = out[:, q * LANES : (q + 1) * LANES]

    def pair_stage(k):
        to_pair(k).wait_recv()
        theirs = core * 2 * group + (1 - far) * group
        mine = core * 2 * group + far * group
        s2[k] = (s1[k, pl.ds(theirs, group)] + r1[k, pl.ds((1 - far) * group, group)]).astype(BF16)
        to_peer(k).start()
        k2[k] = s1[k, pl.ds(mine, group)] + r1[k, pl.ds(far * group, group)]

    def peer_stage(k):
        to_peer(k).wait_recv()
        s3[k] = (k2[k] + r2[k].astype(F32)).astype(BF16)

        @pl.loop(1, heads)
        def _(i):
            to_owner(k, i).start()

        factors[rows_of(h, k)] = s3[k, h]

    def table_stage(k):
        for kind, start in ((0, 2), (1, 4), (2, 6)):
            @pl.when((k >= start) & (k < start + TABLE_PIECES // 2))
            def _():
                for odd in (False, True):
                    t = 2 * (k - start) + (1 if odd else 0)
                    if kind == 0:
                        t_peer(t).wait_recv()
                        t_side(1, t).start()
                        t_side(2, t).start()
                        t_pair(0, t).start()
                    elif kind == 1:
                        t_side(1, t).wait_recv()
                        t_side(2, t).wait_recv()
                        t_relay(t, odd).start()
                        t_pair(1, t).start()
                        t_pair(2, t).start()
                    else:
                        t_relay(t, odd).wait_recv()
                        t_pair(3, t).start()

    grams = (gram_ii, gram_io, gram_oo)
    for ref in grams:
        ref[...] = jnp.zeros_like(ref)
    pair_count[...] = token_pairs(token_row[...], label_row[...], vocab)
    await_others(heads)

    @pl.loop(0, TABLE_PIECES)
    def _(t):
        t_peer(t).start()

    for c in own_to_pair:
        c.start()

    PEER_LAG = 6

    @pl.loop(0, max(steps + PEER_LAG, TABLE_PIECES // 2 + 6))
    def _(k):
        @pl.when(k < steps)
        def _():
            multiply_stage(k)
            to_pair(k).start()

        @pl.when((k >= 1) & (k < steps + 1))
        def _():
            pair_stage(k - 1)

        @pl.when((k >= PEER_LAG) & (k < steps + PEER_LAG))
        def _():
            peer_stage(k - PEER_LAG)

        table_stage(k)

    for c in own_to_pair:
        c.wait_recv()

    @pl.loop(0, 3)
    def _(i):
        add_grams(tables, grams, g ^ i)

    @pl.loop(0, steps)
    def _(k):
        @pl.loop(1, heads)
        def _(i):
            from_holder(k, i).wait_recv()

    widen(factors, flat, spaced, b0, 4)
    near = [factor_products(tables, spaced, b0, c) for c in (g, pair)]
    near.append(factor_products(tables, spaced, b0, peer))

    @pl.loop(0, TABLE_PIECES)
    def _(t):
        for kind in range(4):
            t_pair(kind, t).wait_recv()

    add_grams(tables, grams, g ^ 3)
    near.append(factor_products(tables, spaced, b0, g ^ 3))
    products = [a + b + c + d for a, b, c, d in zip(*near)]
    train(products, flat, b0, loss_out, deltas, tables, grams, pair_count)

    def place(c):
        return (c & 1) * 2 + (c >> 1)

    def to_holder(k, i):
        other = lax.rem(h + i, heads)
        return remote(
            deltas.at[rows_of(other, k)], e.at[place(g), k, h],
            d_send.at[k, other], d_recv.at[k, h], to_head(other),
        )

    def from_owner(k, i):
        other = lax.rem(h + i, heads)
        return remote(
            deltas.at[rows_of(other, k)], e.at[place(g), k, other],
            d_send.at[k, other], d_recv.at[k, other], to_head(other),
        )

    def group_copy(kind, k, receive):
        sender = (peer, pair, pair)[kind] if receive else g
        ref = e.at[place((sender, sender, sender ^ 2)[kind]), k]
        return remote(ref, ref, e_send.at[kind, k], e_recv.at[kind, k], to_client((peer, pair, pair)[kind]))

    @pl.loop(0, steps)
    def _(k):
        @pl.loop(1, heads)
        def _(i):
            to_holder(k, i).start()

    acc[...] = jnp.zeros_like(acc)

    def spread_out(k):
        return pltpu.make_async_copy(
            db.at[k], spread.at[:, pl.ds(pl.multiple_of(k * width, width), width)], o_sem.at[k]
        )

    PEER_AFTER, PAIR_AFTER = 3, 5

    @pl.loop(0, steps + PAIR_AFTER)
    def _(k):
        @pl.when(k < steps)
        def _():
            e[place(g), k, h] = deltas[rows_of(h, k)]

            @pl.loop(1, heads)
            def _(i):
                from_owner(k, i).wait_recv()

            group_copy(0, k, False).start()
            group_copy(1, k, False).start()

        @pl.when((k >= PEER_AFTER) & (k < steps + PEER_AFTER))
        def _():
            group_copy(0, k - PEER_AFTER, True).wait_recv()
            group_copy(2, k - PEER_AFTER, False).start()

        @pl.when(k >= PAIR_AFTER)
        def _():
            j = k - PAIR_AFTER
            group_copy(1, j, True).wait_recv()
            group_copy(2, j, True).wait_recv()
            apart = clients + 4
            for c in range(4):
                for i in range(group):
                    x[pl.ds(c * group + i, PIECE_ROWS, stride=apart), :] = e[c, j, i].astype(F32)
            for q in range(PIECE_ROWS):
                db[j, :, q * LANES : (q + 1) * LANES] = x[q * apart : q * apart + clients, :].astype(BF16)
            spread_out(j).start()
            acc[...] += lax.dot_general(
                wv[j], db[j], (((1,), (1,)), ((), ())), preferred_element_type=F32
            )

    turned = acc[...].T
    for j in range(heads):
        for b in range(units // LANES):
            b1s[j, b * each : (b + 1) * each, :] = turned[
                j * each : (j + 1) * each, b * LANES : (b + 1) * LANES
            ]

    def part_to(i):
        other = lax.rem(h + i, heads)
        return remote(b1s.at[other], b1r.at[h], b_send.at[other], b_recv.at[h], to_head(other))

    def part_from(i):
        other = lax.rem(h + i, heads)
        return remote(b1s.at[other], b1r.at[other], b_send.at[other], b_recv.at[other], to_head(other))

    def sum_to(i):
        other = lax.rem(h + i, heads)
        return remote(tot, b2.at[h], c_send.at[other], c_recv.at[h], to_head(other))

    def sum_from(i):
        other = lax.rem(h + i, heads)
        return remote(tot, b2.at[other], c_send.at[other], c_recv.at[other], to_head(other))

    @pl.loop(1, heads)
    def _(i):
        part_to(i).start()

    @pl.loop(0, steps)
    def _(k):
        to_pair(k).wait_send()
        to_peer(k).wait_send()
        spread_out(k).wait()
        for kind in range(3):
            group_copy(kind, k, False).wait_send()

        @pl.loop(1, heads)
        def _(i):
            to_owner(k, i).wait_send()
            to_holder(k, i).wait_send()

    for c in own_to_pair:
        c.wait_send()
    for c in small_out:
        c.wait()

    @pl.loop(0, TABLE_PIECES)
    def _(t):
        t_peer(t).wait_send()
        t_side(1, t).wait_send()
        t_side(2, t).wait_send()
        t_relay(t, False).wait_send()
        for kind in range(4):
            t_pair(kind, t).wait_send()

    tot[...] = b1s[h]

    @pl.loop(1, heads)
    def _(i):
        part_from(i).wait_recv()
        tot[...] += b1r[lax.rem(h + i, heads)]

    @pl.loop(1, heads)
    def _(i):
        sum_to(i).start()

    b2[h] = tot[...]

    @pl.loop(1, heads)
    def _(i):
        part_to(i).wait_send()
        sum_to(i).wait_send()
        sum_from(i).wait_recv()

    last = pltpu.make_async_copy(b2, back_parts, z_sem)
    last.start()
    last.wait()


def grad_kernel(
    heads, tokens, hidden, spread, back_parts, preact, chosen, loss,
    head_grad, in_grad, losses, turned, hb, stage, ig, g_sem, i_sem,
):
    clients, units = hidden.shape
    each = clients // heads
    slots, _, block = stage.shape
    steps = spread.shape[1] // block
    turned[...] = hidden[...].astype(F32).T.astype(BF16)

    def block_out(k):
        return pltpu.make_async_copy(
            stage.at[lax.rem(k, slots)],
            head_grad.at[:, pl.ds(pl.multiple_of(k * block, block), block)],
            g_sem.at[lax.rem(k, slots)],
        )

    def fill(first, last):
        @pl.loop(first, last)
        def _(k):
            @pl.when(k >= slots)
            def _():
                block_out(k - slots).wait()

            part = spread[:, pl.ds(pl.multiple_of(k * block, block), block)]
            for m in range(0, units, TILE):
                for n in range(0, block, 2 * TILE):
                    stage[lax.rem(k, slots), m : m + TILE, n : n + 2 * TILE] = jnp.dot(
                        turned[m : m + TILE], part[:, n : n + 2 * TILE], preferred_element_type=F32
                    ).astype(BF16)
            block_out(k).start()

    early = min(slots, steps)
    fill(0, early)
    losses[0] = jnp.max(loss[...]) * (1.0 / tokens)
    for j in range(heads):
        for b in range(units // LANES):
            hb[j * each : (j + 1) * each, b * LANES : (b + 1) * LANES] = back_parts[
                j, b * each : (b + 1) * each, :
            ]
    masked = jnp.where(preact[...] > 0, hb[...], 0.0)
    top = masked.astype(BF16)
    rest = masked - top.astype(F32)
    mid = rest.astype(BF16)
    low = (rest - mid.astype(F32)).astype(BF16)
    sel = chosen[...]
    total = jnp.zeros(ig.shape, F32)
    for term in (low, mid, top):
        total += lax.dot_general(sel, term, (((0,), (0,)), ((), ())), preferred_element_type=F32)
    ig[...] = total
    ig_out = pltpu.make_async_copy(ig, in_grad, i_sem)
    ig_out.start()
    fill(early, steps)

    @pl.loop(steps - early, steps)
    def _(k):
        block_out(k).wait()

    ig_out.wait()


def local(
    client_ids, client_table, in_weight, in_bias, head_weight, tokens, labels, byte_table, out_table
):
    heads = lax.axis_size("head")
    groups = lax.axis_size("client")
    assert groups == 4 and tokens.shape[0] == 1 and heads % 4 == 0
    units, columns = head_weight.shape
    clients = client_ids.shape[0]
    embed = client_table.shape[1]
    vocab, share = byte_table.shape
    depth = share * groups
    width = PIECE_ROWS * LANES
    steps = columns // width
    rows = heads * columns // LANES
    group = clients // groups
    each = clients // heads
    part_rows = each * units // LANES
    any_spec = pl.BlockSpec(memory_space=pl.ANY)
    vmem_spec = pl.BlockSpec(memory_space=pltpu.VMEM)
    dma = pltpu.SemaphoreType.DMA

    vmem = pltpu.VMEM
    spread, back_parts, hidden, preact, chosen, loss = pl.pallas_call(
        functools.partial(round_kernel, heads, steps),
        name="round",
        out_shape=[
            jax.ShapeDtypeStruct((clients, columns), BF16),
            jax.ShapeDtypeStruct((heads, part_rows, LANES), F32),
            jax.ShapeDtypeStruct((clients, units), BF16),
            jax.ShapeDtypeStruct((clients, units), F32),
            jax.ShapeDtypeStruct((clients, embed), BF16),
            jax.ShapeDtypeStruct((8, LANES), F32),
        ],
        in_specs=[vmem_spec] * 3 + [any_spec] * 6,
        out_specs=[any_spec] * 5 + [vmem_spec],
        scratch_shapes=[
            vmem((steps, units, width), BF16),
            vmem(client_table.shape, BF16),
            vmem(in_weight.shape, BF16),
            vmem((units,), F32),
            vmem((2, groups, vocab, share), BF16),
            vmem((clients, embed), BF16),
            vmem((clients, units), F32),
            vmem((clients, units), BF16),
            vmem((steps, clients, PIECE_ROWS, LANES), F32),
            vmem((steps, 2 * group, PIECE_ROWS, LANES), F32),
            vmem((steps, group, PIECE_ROWS, LANES), F32),
            vmem((steps, group, PIECE_ROWS, LANES), BF16),
            vmem((steps, group, PIECE_ROWS, LANES), BF16),
            vmem((steps, group, PIECE_ROWS, LANES), BF16),
            vmem((rows, LANES), BF16),
            vmem((rows, LANES), F32),
            vmem((depth, LANES), BF16),
            vmem((rows * LANES // (2 * depth), depth), BF16),
            vmem((vocab, vocab), F32),
            vmem((vocab, vocab), F32),
            vmem((vocab, vocab), F32),
            vmem((vocab, vocab), F32),
            vmem((rows, LANES), BF16),
            vmem((groups, steps, heads, PIECE_ROWS, LANES), BF16),
            vmem((PIECE_ROWS * (clients + 4), LANES), F32),
            vmem((steps, clients, width), BF16),
            vmem((units, clients), F32),
            vmem((heads, part_rows, LANES), F32),
            vmem((heads, part_rows, LANES), F32),
            vmem((part_rows, LANES), F32),
            vmem((heads, part_rows, LANES), F32),
            dma((steps,)), dma((5,)), dma((3,)),
            dma((steps,)), dma((steps,)), dma((steps,)), dma((steps,)),
            dma((steps, heads)), dma((steps, heads)),
            dma((2,)), dma((2,)), dma((4, TABLE_PIECES)), dma((4, TABLE_PIECES)),
            dma((4, TABLE_PIECES)), dma((4, TABLE_PIECES)),
            dma((steps, heads)), dma((steps, heads)),
            dma((3, steps)), dma((3, steps)),
            dma((heads,)), dma((heads,)), dma((heads,)), dma((heads,)), dma((steps,)), dma,
        ],
        compiler_params=pltpu.CompilerParams(
            collective_id=0, has_side_effects=True, vmem_limit_bytes=HIGH_VMEM
        ),
    )(
        client_ids, tokens, labels, client_table, in_weight, in_bias, head_weight,
        byte_table, out_table,
    )

    block = min(1024, columns)
    slots = 4
    head_grad, in_grad, losses = pl.pallas_call(
        functools.partial(grad_kernel, heads, tokens.shape[1]),
        name="grad",
        out_shape=[
            jax.ShapeDtypeStruct((units, columns), BF16),
            jax.ShapeDtypeStruct((embed, units), F32),
            jax.ShapeDtypeStruct((1,), F32),
        ],
        in_specs=[vmem_spec] * 6,
        out_specs=[any_spec, any_spec, pl.BlockSpec(memory_space=pltpu.SMEM)],
        scratch_shapes=[
            vmem((units, clients), BF16),
            vmem((clients, units), F32),
            vmem((slots, units, block), BF16),
            vmem((embed, units), F32),
            dma((slots,)),
            dma,
        ],
        compiler_params=pltpu.CompilerParams(vmem_limit_bytes=HIGH_VMEM),
    )(hidden, spread, back_parts, preact, chosen, loss)
    return head_grad, in_grad, losses


def solution(mesh):
    placed = (
        P(),
        P(),
        P(None, "client"),
        P("client"),
        P("client", "head"),
        P(("head", "client"), None),
        P(("head", "client"), None),
        P(None, "client"),
        P(None, "client"),
    )
    return jax.shard_map(
        local,
        mesh=mesh,
        in_specs=placed,
        out_specs=(P("client", "head"), P(None, "client"), P(("head", "client"))),
        check_vma=False,
    )
```
